128 devices in a mesh: dev: 128 (over y, x, z, core).
Axes of the slice: x: 4, y: 4, z: 4, core: 2. Of those that a mesh axis runs over, the one named last changes fastest.
Arguments:
- dual_blocks: bfloat16 [128, 3072, 3072], P('dev'), as said below
- rigid_modes: float32 [128, 6, 3072], P('dev'), may hold values from -5 to 5
- dual_local: float32 [128, 8, 3072], P('dev'), may hold values from -6 to 6
- coarse_rhs: float32 [128, 6, 8], P('dev'), may hold values from -4608 to 4608
- iface_sizes: int32 [128], P('dev'), may hold values from 1536 to 3072, as said below
- neighbours: int32 [128, 6], P('dev'), may hold values from -1 to 127, as said below
- shared_counts: int32 [128, 6], P('dev'), may hold values from 256 to 512, as said below
- iface_map: int32 [128, 3072], P('dev'), may hold values from -1 to 3071, as said below
- owner: int32 [128], replicated, may hold values from 0 to 127, as said below
Outputs:
- multipliers: float32 [128, 8, 3072], P('dev')
- projected_residual: float32 [128, 8, 3072], P('dev')
The draws below stay inside these ranges and needn't reach their ends.
Inputs may be any that keep to these rules, and one draw needn't show every extreme that they name: `dual_blocks`: each block is symmetric positive definite, and so is each of its leading principal parts. Grid subdomain g is held by slot owner[g] = (g + s) mod 128 for one offset s of the draw, so the subdomains across the faces -x, +x, -y, +y, -z, +z of slot i sit in slots i - 1, i + 1, i - 4, i + 4, i - 16, i + 16, taken mod 128. `neighbours`: the subdomains form a grid of 4 x 4 x 128/16 with g = x + 4 y + 16 z. Row i lists, for the faces -x, +x, -y, +y, -z, +z of the subdomain held in slot i, the grid subdomain across that face, or -1 on the outer boundary; across a face from g the opposite face names g. `shared_counts`: equal on both sides of a shared face; some subdomain has 512 on all its faces. `iface_sizes`: the sum of the slot's shared_counts row; some subdomain has 3072. `iface_map`: for j < iface_sizes[i], entry j is f * 512 + p for the dof at position p of face f of slot i (p below that face's count), each such code once; -1 beyond. The dof at position p of a shared face pairs with the dof at position p of the opposite face of the neighbour.
All inputs are finite; a program needn't handle non-finite values.
Results may differ from the reference program's by a relative error of at most 0.025.
Values sent between devices are 32-bit elements; how exact they have to be, the bound alone decides.
A program may use at most 128 MiB of HBM per device.

```python
import math
import jax
import jax.numpy as jnp
from jax import lax

FACES = 6
MODES = 6
CAP = 512
NMAX = 3072
LOADS = 8
ITERS = 3
NSUB = 128


def grid_links():
    layers = NSUB // 16
    identity = jnp.arange(NSUB, dtype=jnp.int32)
    along_x = identity % 4
    along_y = identity // 4 % 4
    along_z = identity // 16
    columns = [jnp.where(along_x > 0, identity - 1, -1), jnp.where(along_x < 3, identity + 1, -1), jnp.where(along_y > 0, identity - 4, -1), jnp.where(along_y < 3, identity + 4, -1), jnp.where(along_z > 0, identity - 16, -1), jnp.where(along_z < layers - 1, identity + 16, -1)]
    return jnp.stack(columns, axis=1).astype(jnp.int32)


def layout_draw(key):
    base = jax.random.fold_in(key, 7301)
    key_count, key_star, key_owner, key_order = jax.random.split(base, 4)
    links = grid_links()
    drawn = jax.random.randint(key_count, (NSUB, FACES), CAP // 2, CAP + 1, dtype=jnp.int32)
    star = jax.random.randint(key_star, (), 0, NSUB, dtype=jnp.int32)
    drawn = drawn.at[star].set(CAP)
    for lower_face in (0, 2, 4):
        across = links[star, lower_face]
        drawn = drawn.at[jnp.where(across < 0, star, across), lower_face + 1].set(CAP)
    counts = drawn
    for lower_face in (0, 2, 4):
        across = links[:, lower_face]
        mirrored = drawn[jnp.clip(across, 0, NSUB - 1), lower_face + 1]
        counts = counts.at[:, lower_face].set(jnp.where(across < 0, drawn[:, lower_face], mirrored))
    offset = jax.random.randint(key_owner, (), 1, NSUB, dtype=jnp.int32)
    identity = jnp.arange(NSUB, dtype=jnp.int32)
    owner = ((identity + offset) % NSUB).astype(jnp.int32)
    hosted = ((identity - offset + NSUB) % NSUB).astype(jnp.int32)
    slot_links = links[hosted]
    slot_counts = counts[hosted]
    sizes = jnp.sum(slot_counts, axis=1).astype(jnp.int32)
    codes_all = jnp.arange(FACES * CAP, dtype=jnp.int32)
    live_codes = (codes_all % CAP)[None, :] < slot_counts[:, codes_all // CAP]
    slot_keys = jax.random.split(key_order, NSUB)
    shuffles = jax.vmap(lambda slot_key: jax.random.permutation(slot_key, FACES * CAP))(slot_keys).astype(jnp.int32)
    scores = shuffles + jnp.where(live_codes, 0, FACES * CAP).astype(jnp.int32)
    ordered = jnp.argsort(scores, axis=1, stable=True).astype(jnp.int32)
    positions = jnp.arange(NMAX, dtype=jnp.int32)
    iface_map = jnp.where(positions[None, :] < sizes[:, None], ordered, -1).astype(jnp.int32)
    return (owner, sizes, slot_links, slot_counts, iface_map, hosted)


def draw_owner(key, part):
    return layout_draw(key)[0]


def draw_iface_sizes(key, part):
    return layout_draw(key)[1]


def draw_neighbours(key, part):
    return layout_draw(key)[2]


def draw_shared_counts(key, part):
    return layout_draw(key)[3]


def draw_iface_map(key, part):
    return layout_draw(key)[4]


def mode_sample(sample_key, shape):
    values = jnp.clip(jax.random.normal(sample_key, shape, jnp.float32), -4.0, 4.0)
    return values


def draw_rigid_modes(key, part):
    owner, sizes, slot_links, slot_counts, iface_map, hosted = layout_draw(key)
    base = jax.random.fold_in(key, 7303)
    key_common, key_edge, key_own = jax.random.split(base, 3)
    common = mode_sample(key_common, (NSUB, 3, MODES, CAP))
    edge = mode_sample(key_edge, (NSUB, FACES, MODES, CAP))
    own = mode_sample(key_own, (NSUB, MODES, NMAX))
    face_ids = jnp.arange(FACES, dtype=jnp.int32)
    upper = face_ids % 2 == 1
    face_key = jnp.where(upper[None, :], hosted[:, None], slot_links)
    face_key = jnp.clip(face_key, 0, NSUB - 1).astype(jnp.int32)
    axis_ids = (face_ids // 2).astype(jnp.int32)
    face_vals = common[face_key, axis_ids[None, :]]
    face_vals = jnp.where((slot_links >= 0)[:, :, None, None], face_vals, edge)
    flattened = jnp.transpose(face_vals, (0, 2, 1, 3)).reshape(NSUB, MODES, FACES * CAP)
    codes = jnp.clip(iface_map, 0, FACES * CAP - 1).astype(jnp.int32)
    gather_index = jnp.broadcast_to(codes[:, None, :], (NSUB, MODES, NMAX))
    picked = jnp.take_along_axis(flattened, gather_index, axis=2)
    return (picked + 0.25 * own).astype(jnp.float32)


def draw_dual_blocks(key, part):
    slot_keys = jax.random.split(jax.random.fold_in(key, 7302), NSUB)
    spread = 0.3 / math.sqrt(NMAX)

    def single(slot_key):
        key_off, key_diag = jax.random.split(slot_key)
        entries = jax.random.normal(key_off, (NMAX, NMAX), jnp.float32)
        symmetric = (entries + entries.T) * (spread / math.sqrt(2.0))
        diag_vals = jax.random.uniform(key_diag, (NMAX,), jnp.float32, 1.0, 1.5)
        return (symmetric + jnp.diag(diag_vals)).astype(jnp.bfloat16)
    return jax.lax.map(single, slot_keys)


def block_levels(stream_key, shape, shards, smallest, largest):
    loudness, own = 1.0, jax.random.fold_in(stream_key, 6)
    for dim, shards_of in shards:
        steps = jnp.exp(jax.random.uniform(jax.random.fold_in(own, dim), (shards_of,), jnp.float32, smallest / len(shards), largest / len(shards)))
        loudness = loudness * jnp.repeat(steps, shape[dim] // shards_of).reshape([-1 if axis == dim else 1 for axis in range(len(shape))])
    return loudness


def normal_values(stream_key, extent, scale, bound, cuts=(), kind=jnp.bfloat16):
    values = scale * jax.random.normal(stream_key, extent, jnp.float32)
    if cuts:
        values = values * block_levels(stream_key, extent, cuts, -0.22, 0.18)
    return jnp.clip(values, -bound, bound).astype(kind)


def setup_inputs(seed: int = 0) -> dict:
    key_list = jax.random.split(jax.random.key(seed), 10)
    dual_blocks = draw_dual_blocks(jax.random.fold_in(key_list[9], 71), 0)
    rigid_modes = draw_rigid_modes(jax.random.fold_in(key_list[9], 71), 0)
    dual_local = normal_values(key_list[2], (NSUB, LOADS, NMAX), 1.0, 6.0, ((0, 128),), jnp.float32)
    coarse_rhs = normal_values(key_list[3], (NSUB, MODES, LOADS), (NMAX // 4), 4608.0, ((0, 128),), jnp.float32)
    iface_sizes = draw_iface_sizes(jax.random.fold_in(key_list[9], 71), 0)
    neighbours = draw_neighbours(jax.random.fold_in(key_list[9], 71), 0)
    shared_counts = draw_shared_counts(jax.random.fold_in(key_list[9], 71), 0)
    iface_map = draw_iface_map(jax.random.fold_in(key_list[9], 71), 0)
    owner = draw_owner(jax.random.fold_in(key_list[9], 71), 0)
    return {"dual_blocks": dual_blocks, "rigid_modes": rigid_modes, "dual_local": dual_local, "coarse_rhs": coarse_rhs, "iface_sizes": iface_sizes, "neighbours": neighbours, "shared_counts": shared_counts, "iface_map": iface_map, "owner": owner}


OPPOSITE = (1, 0, 3, 2, 5, 4)
HIGHEST_PRECISION = lax.Precision.HIGHEST

def tables(iface_sizes, neighbours, shared_counts, iface_map, owner):
    columns = jnp.arange(NMAX, dtype=jnp.int32)
    live_dofs = columns[None, :] < iface_sizes[:, None]
    dof_codes = jnp.clip(jnp.where(live_dofs, iface_map, 0), 0, FACES * CAP - 1).astype(jnp.int32)
    which_face = dof_codes // CAP
    position = dof_codes % CAP
    face_owner = jnp.take_along_axis(neighbours, which_face, axis=1)
    face_count = jnp.take_along_axis(shared_counts, which_face, axis=1)
    shared = live_dofs & (face_owner >= 0) & (position < face_count)
    weights = jnp.where(shared, 0.5, jnp.where(live_dofs, 1.0, 0.0)).astype(jnp.float32)
    row_index = jnp.broadcast_to(jnp.arange(NSUB, dtype=jnp.int32)[:, None], (NSUB, NMAX))
    targets = jnp.where(live_dofs, dof_codes, FACES * CAP).astype(jnp.int32)
    inverse = jnp.full((NSUB, FACES * CAP), NMAX, jnp.int32)
    inverse = inverse.at[row_index, targets].set(jnp.broadcast_to(columns[None, :], (NSUB, NMAX)), mode='drop')
    partner_slot = jnp.where(neighbours >= 0, owner[jnp.clip(neighbours, 0, NSUB - 1)], 0).astype(jnp.int32)
    face_mask = ((neighbours >= 0)[:, :, None] & (jnp.arange(CAP, dtype=jnp.int32)[None, None, :] < shared_counts[:, :, None])).astype(jnp.float32)
    return (live_dofs, dof_codes, shared, weights, inverse, partner_slot, face_mask)

def to_faces(values, inverse):
    padded = jnp.concatenate([values, jnp.zeros((values.shape[0], values.shape[1], 1), values.dtype)], axis=2)
    gather_index = jnp.broadcast_to(inverse[:, None, :], (values.shape[0], values.shape[1], FACES * CAP))
    return jnp.take_along_axis(padded, gather_index, axis=2).reshape(values.shape[0], values.shape[1], FACES, CAP)

def partner_faces(face_vals, partner_slot, face_mask):
    opposite = jnp.array(OPPOSITE, jnp.int32)
    swapped = jnp.transpose(face_vals, (0, 2, 1, 3))
    picked = swapped[partner_slot, opposite[None, :]]
    return picked * face_mask[:, :, None, :]

def to_dofs(far_faces, dof_codes, shared):
    flattened = jnp.transpose(far_faces, (0, 2, 1, 3)).reshape(far_faces.shape[0], far_faces.shape[2], FACES * CAP)
    gather_index = jnp.broadcast_to(dof_codes[:, None, :], (far_faces.shape[0], far_faces.shape[2], NMAX))
    return jnp.take_along_axis(flattened, gather_index, axis=2) * shared.astype(jnp.float32)[:, None, :]

def assemble(values, layout):
    live_dofs, dof_codes, shared, weights, inverse, partner_slot, face_mask = layout
    far_faces = partner_faces(to_faces(values, inverse), partner_slot, face_mask)
    return live_dofs.astype(jnp.float32)[:, None, :] * (values - to_dofs(far_faces, dof_codes, shared))

def dual_products(dual_blocks, vectors):

    def single(operands):
        dual_block, vector = operands
        return lax.dot_general(vector.astype(jnp.bfloat16).astype(jnp.float32), dual_block.astype(jnp.float32), (((1,), (1,)), ((), ())), preferred_element_type=jnp.float32)
    return lax.map(single, (dual_blocks, vectors))

def solve_coarse(factor, vector):
    middle = lax.linalg.triangular_solve(factor, vector, left_side=True, lower=True)
    return lax.linalg.triangular_solve(factor, middle, left_side=True, lower=True, transpose_a=True)

def weighted_inner(weights, left_vec, right_vec):
    return jnp.sum(weights[:, None, :] * left_vec * right_vec, axis=(0, 2))

def reference(dual_blocks, rigid_modes, dual_local, coarse_rhs, iface_sizes, neighbours, shared_counts, iface_map, owner):
    layout = tables(iface_sizes, neighbours, shared_counts, iface_map, owner)
    live_dofs, dof_codes, shared, weights, inverse, partner_slot, face_mask = layout
    live_float = live_dofs.astype(jnp.float32)
    modes_live = rigid_modes * live_float[:, None, :]
    own_modes = to_faces(modes_live, inverse)
    far_modes = partner_faces(own_modes, partner_slot, face_mask)
    diagonal = jnp.einsum('iaj,ibj->iab', modes_live, modes_live, precision=HIGHEST_PRECISION)
    coupling = -jnp.einsum('iafp,ifbp->ifab', own_modes, far_modes, precision=HIGHEST_PRECISION)
    slot_index = jnp.arange(NSUB, dtype=jnp.int32)
    coarse_blocks = jnp.zeros((NSUB, MODES, NSUB, MODES), jnp.float32)
    coarse_blocks = coarse_blocks.at[slot_index, :, slot_index, :].set(diagonal)
    coarse_blocks = coarse_blocks.at[slot_index[:, None], :, partner_slot, :].add(coupling)
    factor = jnp.linalg.cholesky(coarse_blocks.reshape(NSUB * MODES, NSUB * MODES))

    def modes_apply(solution):
        stacked = solution.reshape(NSUB, MODES, LOADS)
        own_part = jnp.einsum('iaj,ial->ilj', modes_live, stacked, precision=HIGHEST_PRECISION)
        return assemble(own_part, layout)

    def project(residual):
        coarse_all = jnp.einsum('iaj,ilj->ial', modes_live, residual, precision=HIGHEST_PRECISION).reshape(NSUB * MODES, LOADS)
        projected = residual - modes_apply(solve_coarse(factor, coarse_all))
        return (projected, weighted_inner(weights, projected, projected))

    def dual_apply(vector):
        return assemble(dual_products(dual_blocks, vector), layout)
    dual_rhs = assemble(dual_local, layout)
    multipliers = modes_apply(solve_coarse(factor, coarse_rhs.reshape(NSUB * MODES, LOADS)))
    residual = dual_rhs - dual_apply(multipliers)
    projected, norm_sq = project(residual)
    direction = projected
    for step_index in range(ITERS):
        applied = dual_apply(direction)
        step_size = norm_sq / weighted_inner(weights, direction, applied)
        multipliers = multipliers + step_size[None, :, None] * direction
        residual = residual - step_size[None, :, None] * applied
        projected, norm_next = project(residual)
        direction = projected + (norm_next / norm_sq)[None, :, None] * direction
        norm_sq = norm_next
    return (multipliers, projected)
```

```python
import functools

import jax
import jax.numpy as jnp
from jax import lax
from jax.experimental import pallas as pl
from jax.experimental.pallas import tpu as pltpu
from jax.sharding import PartitionSpec as P

FACES = 6
MODES = 6
CAP = 512
NMAX = 3072
LOADS = 8
CHUNKS = NMAX // 128
ITERS = 3
DEVICES = 128
OPPOSITE = (1, 0, 3, 2, 5, 4)
FACE_STEPS = (-1, 1, -4, 4, -16, 16)
HIGHEST = lax.Precision.HIGHEST
F32 = jnp.float32
BF16 = jnp.bfloat16
MESH = pl.DeviceIdType.MESH


def iota(shape, dim):
    return lax.broadcasted_iota(jnp.int32, shape, dim)


def lane_take(values, lanes):
    return jnp.take_along_axis(values, lanes, axis=1, mode="promise_in_bounds")


def permuted_chunk(src, index_row):
    index = jnp.broadcast_to(index_row, (8, 128))
    chunk = index >> 7
    lanes = index & 127
    out = jnp.zeros((8, 128), F32)
    for s in range(CHUNKS):
        piece = lane_take(src[:, s * 128 : (s + 1) * 128], lanes)
        out = jnp.where(chunk == s, piece, out)
    return out


def neighbour(me, step):
    return lax.rem(me + step + DEVICES, DEVICES)


def face_slice(face):
    return pl.ds(face * CAP, CAP)


def greet(partners):
    barrier = pltpu.get_barrier_semaphore()
    for partner in partners:
        pl.semaphore_signal(barrier, inc=1, device_id=(partner,), device_id_type=MESH)
    pl.semaphore_wait(barrier, len(partners))


def remote(src, dst, send, recv, device):
    return pltpu.make_async_remote_copy(
        src_ref=src, dst_ref=dst, send_sem=send, recv_sem=recv,
        device_id=(device,), device_id_type=MESH,
    )


def split3(x):
    hi = x.astype(BF16).astype(F32)
    rest = x - hi
    mid = rest.astype(BF16).astype(F32)
    return hi, mid, rest - mid


def setup_kernel(
    counts, links, map_ref, modes_ref, rhs_ref, goal_ref,
    rows_out, basis_out, modes_out, rhs_out, inverse_out,
    padded, own, far, basis, gathered,
    halo_send, halo_recv, y_send, y_recv, x_send, x_recv, z_send, z_recv, c_send, c_recv,
):
    me = lax.axis_index("dev")
    core = lax.rem(me, 2)
    z = lax.rem(me // 2, 4)
    x = lax.rem(me // 8, 4)
    y = me // 32

    def at(y_, x_, z_, c_):
        return ((y_ * 4 + x_) * 4 + z_) * 2 + c_

    def turn(value, by):
        return lax.rem(value + by, 4)

    partners = [neighbour(me, step) for step in FACE_STEPS]
    partners += [at(turn(y, j), x, z, core) for j in (1, 2, 3)]
    partners += [at(y, turn(x, j), z, core) for j in (1, 2, 3)]
    partners += [at(y, x, turn(z, j), core) for j in (1, 2, 3)]
    partners += [at(y, x, z, 1 - core)]
    greet(partners)

    codes = map_ref[...]
    high = jnp.where(codes >= 0, codes >> 7, -1)
    low = jnp.where(codes >= 0, codes & 127, -1)
    column = iota((32, NMAX), 1)
    here = jnp.broadcast_to(high, (32, NMAX)) == iota((32, NMAX), 0)
    coarse_digit = jnp.where(here, column >> 6, 0).astype(F32).astype(BF16)
    fine_digit = jnp.where(here, column & 63, 0).astype(F32).astype(BF16)
    spots = (
        jnp.broadcast_to(low, (128, NMAX)) == iota((128, NMAX), 0)
    ).astype(F32).astype(BF16)
    digits = lax.dot_general(
        jnp.concatenate([coarse_digit, fine_digit], axis=0), spots,
        (((1,), (1,)), ((), ())), preferred_element_type=F32,
    )
    inverse = (digits[:32] * 64.0 + digits[32:]).astype(jnp.int32)
    inverse_out[...] = inverse[:CHUNKS]

    padded[...] = jnp.zeros_like(padded)
    padded[0:MODES, :] = modes_ref[0]
    for r in range(CHUNKS):
        face = r // 4
        live = iota((8, 128), 1) + (r % 4) * 128 < counts[0, face]
        row = inverse_out[r : r + 1, :]
        own[0, :, r * 128 : (r + 1) * 128] = jnp.where(live, permuted_chunk(padded, row), 0.0)
        own[1, :, r * 128 : (r + 1) * 128] = jnp.where(live, permuted_chunk(rhs_ref.at[0], row), 0.0)

    copies = [
        remote(
            own.at[:, :, face_slice(face)], far.at[:, :, face_slice(OPPOSITE[face])],
            halo_send.at[face], halo_recv.at[OPPOSITE[face]], neighbour(me, FACE_STEPS[face]),
        )
        for face in range(FACES)
    ]
    for copy in copies:
        copy.start()
    basis[...] = jnp.zeros_like(basis)
    basis[48:56, :] = own[0]
    modes_out[...] = own[0]
    for copy in copies:
        copy.wait()
    for face in range(FACES):
        limit = jnp.where(links[0, face] >= 0, counts[0, face], 0)
        shared = iota((8, CAP), 1) < limit
        lanes = face_slice(face)
        basis[8 * face : 8 * face + 8, lanes] = jnp.where(shared, -far[0, :, lanes], 0.0)
        rhs_out[:, lanes] = own[1, :, lanes] - jnp.where(shared, far[1, :, lanes], 0.0)

    row_block = lax.dot_general(
        own[0], basis[...], (((1,), (1,)), ((), ())),
        precision=HIGHEST, preferred_element_type=F32,
    )
    row_block = jnp.where(iota((8, 128), 0) == 6, jnp.broadcast_to(goal_ref[...], (8, 128)), row_block)
    gathered[y, x, z, core] = row_block
    phases = (
        (y, y_send, y_recv, lambda: gathered.at[y, x, z, core], lambda k: at(k, x, z, core)),
        (x, x_send, x_recv, lambda: gathered.at[:, x, z, core], lambda k: at(y, k, z, core)),
        (z, z_send, z_recv, lambda: gathered.at[:, :, z, core], lambda k: at(y, x, k, core)),
    )
    for place, send, recv, part, device in phases:
        copies = [
            remote(part(), part(), send.at[j - 1], recv.at[j - 1], device(turn(place, j)))
            for j in (1, 2, 3)
        ]
        for copy in copies:
            copy.start()
        if place is y:
            top = basis[0:64, :]
            hi = top.astype(BF16)
            basis_out[0:64, :] = hi
            basis_out[64:128, :] = (top - hi.astype(F32)).astype(BF16)
            basis_out[128:192, :] = hi
        for copy in copies:
            copy.wait()
    copy = remote(
        gathered.at[:, :, :, core], gathered.at[:, :, :, core],
        c_send, c_recv, at(y, x, z, 1 - core),
    )
    copy.start()
    copy.wait()
    rows_out[...] = gathered[...].reshape(DEVICES * 8, 128)


def invert_together(blocks, layers):
    lane = iota((8, 128), 1)
    sub = iota((8, 128), 0)

    def node(n, carry):
        base = pl.multiple_of(n * 8, 8)
        results = []
        for layer in layers:
            panel = blocks[layer, pl.ds(base, 8), :]
            cols = [lane_take(panel, jnp.full((8, 128), base + k, jnp.int32)) for k in range(MODES)]
            inside = (lane >> 3) == n
            work = jnp.where(inside, jnp.where(lane - base == sub, 1.0, 0.0), panel)
            for k in range(MODES):
                inv = 1.0 / jnp.broadcast_to(cols[k][k : k + 1, :], (8, 128))
                lift = jnp.where(sub == k, cols[k] - 1.0, cols[k])
                work = work - lift * (jnp.broadcast_to(work[k : k + 1, :], (8, 128)) * inv)
                for j in range(k + 1, MODES):
                    cols[j] = cols[j] - lift * (jnp.broadcast_to(cols[j][k : k + 1, :], (8, 128)) * inv)
            results.append(work)
        for layer, work in zip(layers, results):
            inside = (lane >> 3) == n
            spread = [jnp.broadcast_to(work[k : k + 1, :], (8, 128)) for k in range(MODES)]
            for m in range(16):
                row = blocks[layer, m * 8 : (m + 1) * 8, :]
                out = jnp.where(inside, 0.0, row)
                for k in range(MODES):
                    out = out - lane_take(row, jnp.full((8, 128), base + k, jnp.int32)) * spread[k]
                blocks[layer, m * 8 : (m + 1) * 8, :] = out
            blocks[layer, pl.ds(base, 8), :] = work
        return carry

    lax.fori_loop(0, 16, node, 0)


def mm(a, b):
    return jnp.dot(a, b, precision=HIGHEST, preferred_element_type=F32)


def coarse_kernel(owner, links, place, rows, rows_kept_out, solver_out, blocks, up, down, fold, sel):
    lane = iota((8, 128), 1)
    sub = iota((8, 128), 0)
    offset = owner[0]
    me = place[0]

    def layer_rows(layer, carry):
        for n in range(16):
            slot = (layer * 16 + n + offset) & (DEVICES - 1)
            tile = rows[pl.ds(pl.multiple_of(slot * 8, 8), 8), :]
            real = sub < MODES
            apart = (lane >> 3) - n
            within = lane & 7
            face = jnp.where(apart == 0, 6, jnp.where(apart == -1, 0, jnp.where(
                apart == 1, 1, jnp.where(apart == -4, 2, jnp.where(apart == 4, 3, 7)))))
            linked = (face < 7) & real & (within < MODES)
            block = jnp.where(linked, lane_take(tile, face * 8 + within), 0.0)
            pad = (apart == 0) & (within == sub) & (sub >= MODES)
            blocks[layer, n * 8 : n * 8 + 8, :] = jnp.where(pad, 1.0, block)
            here = (apart == 0) & real & (within < MODES)
            up[layer, n * 8 : n * 8 + 8, :] = jnp.where(here, lane_take(tile, 40 + within), 0.0)
            down[layer, n * 8 : n * 8 + 8, :] = jnp.where(here, lane_take(tile, 32 + within), 0.0)
        return carry

    lax.fori_loop(0, 8, layer_rows, 0)

    own = (me - offset) & (DEVICES - 1)
    for f in range(7):
        target = own if f == 6 else links[0, f]
        for layer in range(8):
            hit = ((lane >> 3) + 16 * layer == target) & ((lane & 7) == sub) & (sub < MODES)
            sel[layer, 8 * f : 8 * f + 8, :] = jnp.where(hit, 1.0, 0.0)
    for layer in range(8):
        sel[layer, 56:64, :] = jnp.zeros((8, 128), F32)

    for k in range(3):
        low, high = k, 7 - k
        invert_together(blocks, (low, high))
        fold[low] = mm(blocks[low], up[low])
        fold[high] = mm(blocks[high], down[high])
        blocks[low + 1] = blocks[low + 1] - mm(down[low + 1], fold[low])
        blocks[high - 1] = blocks[high - 1] - mm(up[high - 1], fold[high])
        sel[low + 1] = sel[low + 1] - mm(sel[low], fold[low])
        sel[high - 1] = sel[high - 1] - mm(sel[high], fold[high])
    invert_together(blocks, (3,))
    fold[3] = mm(blocks[3], up[3])
    blocks[4] = blocks[4] - mm(down[4], fold[3])
    sel[4] = sel[4] - mm(sel[3], fold[3])
    invert_together(blocks, (4,))
    sel[4] = mm(sel[4], blocks[4])
    for k in range(3, -1, -1):
        sel[k] = mm(sel[k] - mm(sel[k + 1], down[k + 1]), blocks[k])
        if k < 3:
            j = 7 - k
            sel[j] = mm(sel[j] - mm(sel[j - 1], up[j - 1]), blocks[j])

    parts = []
    for layer in range(8):
        parts.append(jnp.concatenate(split3(sel[layer]), axis=0).astype(BF16))
    row = iota((128, 128), 0)
    col = iota((128, 128), 1)
    for k in range(MODES):
        total = jnp.zeros((192, 128), F32)
        for layer in range(8):
            slot = ((row >> 3) + 16 * layer + offset) & (DEVICES - 1)
            hot = jnp.where(((row & 7) == k) & (slot == col), 1.0, 0.0).astype(BF16)
            total = total + jnp.dot(parts[layer], hot, preferred_element_type=F32)
        values = total[0:64] + total[64:128] + total[128:192]
        hi = values.astype(BF16)
        solver_out[k * 64 : (k + 1) * 64, 0:128] = hi
        solver_out[k * 64 : (k + 1) * 64, 128:256] = hi
        solver_out[k * 64 : (k + 1) * 64, 256:384] = (values - hi.astype(F32)).astype(BF16)
    rows_kept_out[...] = rows[pl.ds(6, DEVICES, stride=8), :]


def cg_kernel(
    counts, links, map_ref, inverse, modes, rhs, basis, solver, goal, dual_hbm,
    lambda_out, residual_out,
    dual, vec, low_vec, prod, image, far, lam, direction, applied, coarse, live, omega, table,
    dual_sem, halo_send, halo_recv, near_send, near_recv, wide_send, wide_recv,
):
    me = lax.axis_index("dev")
    q = lax.rem(me, 8)
    h = me // 8
    near = [h * 8 + lax.rem(q + j, 8) for j in range(1, 8)]
    wide = [lax.rem(h + j, 16) * 8 + q for j in range(1, 16)]
    load = pltpu.make_async_copy(dual_hbm.at[0], dual, dual_sem)
    load.start()
    greet([neighbour(me, step) for step in FACE_STEPS] + near + wide)

    lane = iota((8, 128), 1)
    sub = iota((8, 128), 0)
    for face in range(FACES):
        spot = iota((8, CAP), 1)
        alive = jnp.where(spot < counts[0, face], 1.0, 0.0)
        limit = jnp.where(links[0, face] >= 0, counts[0, face], 0)
        both = jnp.where(spot < limit, 1.0, 0.0)
        live[:, face_slice(face)] = both
        omega[:, face_slice(face)] = alive - 0.5 * both

    def coarse_solve(table_rows):
        hi = table_rows.astype(BF16)
        lo = (table_rows - hi.astype(F32)).astype(BF16)
        stacked = jnp.concatenate([hi, lo, hi], axis=0)
        out = jnp.dot(solver[...], stacked, preferred_element_type=F32)
        total = jnp.zeros((64, 128), F32)
        for k in range(MODES):
            total = jnp.where((iota((64, 128), 1) & 15) == k, out[k * 64 : (k + 1) * 64], total)
        top = total.astype(BF16)
        rest = (total - top.astype(F32)).astype(BF16)
        pair = jnp.concatenate([top, rest], axis=1)
        triple = jnp.concatenate([pair, pair, pair], axis=0)
        group = jnp.where(
            ((iota((8, 256), 1) & 127) >> 4) == iota((8, 256), 0), 1.0, 0.0
        ).astype(BF16)
        return lax.dot_general(
            group, triple, (((1,), (1,)), ((), ())), preferred_element_type=F32
        )

    def expand(z3):
        top = z3.astype(BF16).astype(F32)
        packed = jnp.where(iota((8, 192), 1) < 128, top, z3 - top).astype(BF16)
        return jnp.dot(packed, basis[...], preferred_element_type=F32)

    def dual_apply():
        def to_columns(o, carry):
            lanes = pl.ds(pl.multiple_of(o * 128, 128), 128)
            low_vec[:, lanes] = permuted_chunk(vec, map_ref[:, lanes]).astype(BF16)
            return carry

        lax.fori_loop(0, CHUNKS, to_columns, 0)

        def product(n, carry):
            lanes = pl.ds(pl.multiple_of(n * 512, 512), 512)
            prod[:, lanes] = jnp.dot(low_vec[...], dual[:, lanes], preferred_element_type=F32)
            return carry

        lax.fori_loop(0, NMAX // 512, product, 0)

        def to_faces(r, carry):
            lanes = pl.ds(pl.multiple_of(r * 128, 128), 128)
            image[:, lanes] = permuted_chunk(prod, inverse[pl.ds(r, 1), :])
            return carry

        lax.fori_loop(0, CHUNKS, to_faces, 0)
        copies = [
            remote(
                image.at[:, face_slice(face)], far.at[:, face_slice(OPPOSITE[face])],
                halo_send.at[face], halo_recv.at[OPPOSITE[face]],
                neighbour(me, FACE_STEPS[face]),
            )
            for face in range(FACES)
        ]
        for copy in copies:
            copy.start()
        for copy in copies:
            copy.wait()
        shared = live[...]
        alive = omega[...] + 0.5 * shared
        prod[...] = jnp.where(alive > 0.0, image[...], 0.0) - jnp.where(shared > 0.0, far[...], 0.0)

    def gather_sums(parity, columns):
        tile = jnp.zeros((8, 128), F32)
        for k, values in enumerate(columns):
            tile = jnp.where((lane & 15) == k, values, tile)
        mine = jnp.sum(jnp.where((lane >> 4) == sub, tile, 0.0), axis=0, keepdims=True)
        table[parity, h, pl.ds(q, 1), :] = mine
        row = lambda: table.at[parity, h, pl.ds(q, 1), :]
        copies = [
            remote(row(), row(), near_send.at[parity, j], near_recv.at[parity, j], near[j])
            for j in range(7)
        ]
        for copy in copies:
            copy.start()
        for copy in copies:
            copy.wait()
        copies = [
            remote(
                table.at[parity, h], table.at[parity, h],
                wide_send.at[parity, j], wide_recv.at[parity, j], wide[j],
            )
            for j in range(15)
        ]
        for copy in copies:
            copy.start()
        for copy in copies:
            copy.wait()
        return table[parity].reshape(DEVICES, 128)

    def mode_sums(values):
        return [
            jnp.sum(modes[a : a + 1, :] * values, axis=1, keepdims=True) for a in range(MODES)
        ]

    def summed(left, right):
        return jnp.sum(omega[...] * left * right, axis=1, keepdims=True)

    def total_of(totals, k):
        return jnp.sum(jnp.where(lane == 16 * sub + k, totals, 0.0), axis=1, keepdims=True)

    start = expand(coarse_solve(goal[...]))
    lam[...] = start
    vec[...] = start
    load.wait()
    dual_apply()
    residual = rhs[...] - prod[...]
    z3 = coarse_solve(gather_sums(0, mode_sums(residual)))
    vec[...] = residual - expand(z3)
    direction[...] = jnp.zeros_like(direction)
    applied[...] = jnp.zeros_like(applied)
    coarse[...] = jnp.zeros_like(coarse)

    def iteration(step, carry):
        rho_old, curve_old = carry
        dual_apply()
        w = vec[...]
        columns = mode_sums(prod[...]) + [
            summed(w, w), summed(w, prod[...]), summed(w, applied[...]),
            summed(direction[...], prod[...]),
        ]
        rows = gather_sums(lax.rem(step, 2), columns)
        totals = jnp.broadcast_to(jnp.sum(rows, axis=0, keepdims=True), (8, 128))
        rho = total_of(totals, 6)
        ratio = rho / rho_old
        curve = (
            total_of(totals, 7) + ratio * (total_of(totals, 8) + total_of(totals, 9))
            + ratio * ratio * curve_old
        )
        length = rho / curve
        z3 = coarse_solve(rows) + ratio * coarse[...]
        coarse[...] = z3
        image_of = prod[...] + ratio * applied[...]
        applied[...] = image_of
        way = vec[...] + ratio * direction[...]
        direction[...] = way
        lam[...] = lam[...] + length * way
        vec[...] = vec[...] - length * (image_of - expand(z3))
        return rho, curve

    far_off = jnp.full((8, 1), jnp.inf, F32)
    lax.fori_loop(1, ITERS + 1, iteration, (far_off, jnp.zeros((8, 1), F32)))

    def to_outputs(o, carry):
        lanes = pl.ds(pl.multiple_of(o * 128, 128), 128)
        row = map_ref[:, lanes]
        lambda_out[0, :, lanes] = permuted_chunk(lam, row)
        residual_out[0, :, lanes] = permuted_chunk(vec, row)
        return carry

    lax.fori_loop(0, CHUNKS, to_outputs, 0)


VM = pl.BlockSpec(memory_space=pltpu.VMEM)
SM = pl.BlockSpec(memory_space=pltpu.SMEM)
DMA = pltpu.SemaphoreType.DMA


def sds(shape, dtype=F32):
    return jax.ShapeDtypeStruct(shape, dtype)


def per_device(
    dual_blocks, rigid_modes, dual_local, coarse_rhs,
    iface_sizes, neighbours, shared_counts, iface_map, owner,
):
    goal_row = jnp.pad(coarse_rhs[0].T, ((0, 0), (0, 16 - MODES))).reshape(1, 128)
    rows, basis, modes, rhs, inverse = pl.pallas_call(
        setup_kernel,
        out_shape=(
            sds((DEVICES * 8, 128)), sds((192, NMAX), BF16), sds((8, NMAX)), sds((8, NMAX)),
            sds((CHUNKS, 128), jnp.int32),
        ),
        in_specs=[SM, SM, VM, VM, VM, VM],
        out_specs=(VM,) * 5,
        scratch_shapes=[
            pltpu.VMEM((8, NMAX), F32), pltpu.VMEM((2, 8, NMAX), F32),
            pltpu.VMEM((2, 8, NMAX), F32), pltpu.VMEM((128, NMAX), F32),
            pltpu.VMEM((4, 4, 4, 2, 8, 128), F32),
            DMA((6,)), DMA((6,)), DMA((3,)), DMA((3,)), DMA((3,)), DMA((3,)),
            DMA((3,)), DMA((3,)), DMA, DMA,
        ],
        compiler_params=pltpu.CompilerParams(
            collective_id=0, has_side_effects=True, vmem_limit_bytes=40 << 20
        ),
        name="setup",
    )(shared_counts, neighbours, iface_map, rigid_modes, dual_local, goal_row)

    place = lax.axis_index("dev").astype(jnp.int32).reshape(1)
    goal, solver = pl.pallas_call(
        coarse_kernel,
        out_shape=(sds((DEVICES, 128)), sds((64 * MODES, 384), BF16)),
        in_specs=[SM, SM, SM, VM],
        out_specs=(VM, VM),
        scratch_shapes=[
            pltpu.VMEM((8, 128, 128), F32), pltpu.VMEM((8, 128, 128), F32),
            pltpu.VMEM((8, 128, 128), F32), pltpu.VMEM((8, 128, 128), F32),
            pltpu.VMEM((8, 64, 128), F32),
        ],
        compiler_params=pltpu.CompilerParams(vmem_limit_bytes=40 << 20),
        name="coarse",
    )(owner, neighbours, place, rows)

    return pl.pallas_call(
        cg_kernel,
        out_shape=(sds((1, LOADS, NMAX)), sds((1, LOADS, NMAX))),
        in_specs=[SM, SM] + [VM] * 7 + [pl.BlockSpec(memory_space=pl.ANY)],
        out_specs=(VM, VM),
        scratch_shapes=[
            pltpu.VMEM((NMAX, NMAX), BF16), pltpu.VMEM((8, NMAX), F32),
            pltpu.VMEM((8, NMAX), BF16),
        ] + [pltpu.VMEM((8, NMAX), F32)] * 6 + [
            pltpu.VMEM((8, 192), F32), pltpu.VMEM((8, NMAX), F32), pltpu.VMEM((8, NMAX), F32),
            pltpu.VMEM((2, 16, 8, 128), F32),
            DMA, DMA((6,)), DMA((6,)), DMA((2, 7)), DMA((2, 7)), DMA((2, 15)), DMA((2, 15)),
        ],
        compiler_params=pltpu.CompilerParams(
            collective_id=1, has_side_effects=True, vmem_limit_bytes=56 << 20
        ),
        name="gradients",
    )(
        shared_counts, neighbours, iface_map, inverse, modes, rhs, basis, solver, goal, dual_blocks
    )


def solution(mesh):
    in_specs = (
        P("dev", None, None), P("dev", None, None), P("dev", None, None), P("dev", None, None),
        P("dev"), P("dev", None), P("dev", None), P("dev", None), P(),
    )
    out_specs = (P("dev", None, None), P("dev", None, None))
    return jax.shard_map(
        per_device, mesh=mesh, in_specs=in_specs, out_specs=out_specs, check_vma=False
    )
```

```python
import functools

import jax
import jax.numpy as jnp
from jax import lax
from jax.experimental import pallas as pl
from jax.experimental.pallas import tpu as pltpu
from jax.sharding import PartitionSpec as P

FACES = 6
MODES = 6
CAP = 512
NMAX = 3072
LOADS = 8
CHUNKS = NMAX // 128
ITERS = 3
DEVICES = 128
OPPOSITE = (1, 0, 3, 2, 5, 4)
FACE_STEPS = (-1, 1, -4, 4, -16, 16)
HIGHEST = lax.Precision.HIGHEST
F32 = jnp.float32
BF16 = jnp.bfloat16
MESH = pl.DeviceIdType.MESH


def iota(shape, dim):
    return lax.broadcasted_iota(jnp.int32, shape, dim)


def lane_take(values, lanes):
    return jnp.take_along_axis(values, lanes, axis=1, mode="promise_in_bounds")


def permuted_chunk(src, index_row):
    index = jnp.broadcast_to(index_row, (8, 128))
    chunk = index >> 7
    lanes = index & 127
    out = jnp.zeros((8, 128), F32)
    for s in range(CHUNKS):
        piece = lane_take(src[:, s * 128 : (s + 1) * 128], lanes)
        out = jnp.where(chunk == s, piece, out)
    return out


def neighbour(me, step):
    return lax.rem(me + step + DEVICES, DEVICES)


def face_slice(face):
    return pl.ds(face * CAP, CAP)


def greet(partners):
    barrier = pltpu.get_barrier_semaphore()
    for partner in partners:
        pl.semaphore_signal(barrier, inc=1, device_id=(partner,), device_id_type=MESH)
    pl.semaphore_wait(barrier, len(partners))


def remote(src, dst, send, recv, device):
    return pltpu.make_async_remote_copy(
        src_ref=src, dst_ref=dst, send_sem=send, recv_sem=recv,
        device_id=(device,), device_id_type=MESH,
    )


def split3(x):
    hi = x.astype(BF16).astype(F32)
    rest = x - hi
    mid = rest.astype(BF16).astype(F32)
    return hi, mid, rest - mid


def setup_kernel(
    counts, links, map_ref, modes_ref, rhs_ref, goal_ref,
    rows_out, basis_out, modes_out, edge_out, rhs_out, inverse_out,
    padded, own, far, basis, gathered,
    halo_send, halo_recv, y_send, y_recv, x_send, x_recv, z_send, z_recv, c_send, c_recv,
):
    me = lax.axis_index("dev")
    core = lax.rem(me, 2)
    z = lax.rem(me // 2, 4)
    x = lax.rem(me // 8, 4)
    y = me // 32

    def at(y_, x_, z_, c_):
        return ((y_ * 4 + x_) * 4 + z_) * 2 + c_

    def turn(value, by):
        return lax.rem(value + by, 4)

    partners = [neighbour(me, step) for step in FACE_STEPS]
    partners += [at(turn(y, j), x, z, core) for j in (1, 2, 3)]
    partners += [at(y, turn(x, j), z, core) for j in (1, 2, 3)]
    partners += [at(y, x, turn(z, j), core) for j in (1, 2, 3)]
    partners += [at(y, x, z, 1 - core)]
    greet(partners)

    codes = map_ref[...]
    high = jnp.where(codes >= 0, codes >> 7, -1)
    low = jnp.where(codes >= 0, codes & 127, -1)
    column = iota((32, NMAX), 1)
    here = jnp.broadcast_to(high, (32, NMAX)) == iota((32, NMAX), 0)
    coarse_digit = jnp.where(here, column >> 6, 0).astype(F32).astype(BF16)
    fine_digit = jnp.where(here, column & 63, 0).astype(F32).astype(BF16)
    spots = (
        jnp.broadcast_to(low, (128, NMAX)) == iota((128, NMAX), 0)
    ).astype(F32).astype(BF16)
    digits = lax.dot_general(
        jnp.concatenate([coarse_digit, fine_digit], axis=0), spots,
        (((1,), (1,)), ((), ())), preferred_element_type=F32,
    )
    inverse = (digits[:32] * 64.0 + digits[32:]).astype(jnp.int32)
    inverse_out[...] = inverse[:CHUNKS]

    padded[...] = jnp.zeros_like(padded)
    padded[0:MODES, :] = modes_ref[0]
    for r in range(CHUNKS):
        face = r // 4
        live = iota((8, 128), 1) + (r % 4) * 128 < counts[0, face]
        row = inverse_out[r : r + 1, :]
        own[0, :, r * 128 : (r + 1) * 128] = jnp.where(live, permuted_chunk(padded, row), 0.0)
        own[1, :, r * 128 : (r + 1) * 128] = jnp.where(live, permuted_chunk(rhs_ref.at[0], row), 0.0)

    copies = [
        remote(
            own.at[:, :, face_slice(face)], far.at[:, :, face_slice(OPPOSITE[face])],
            halo_send.at[face], halo_recv.at[OPPOSITE[face]], neighbour(me, FACE_STEPS[face]),
        )
        for face in range(FACES)
    ]
    for copy in copies:
        copy.start()
    basis[...] = jnp.zeros_like(basis)
    basis[48:56, :] = own[0]
    modes_out[...] = own[0]
    for copy in copies:
        copy.wait()
    for face in range(FACES):
        limit = jnp.where(links[0, face] >= 0, counts[0, face], 0)
        shared = iota((8, CAP), 1) < limit
        lanes = face_slice(face)
        edge = jnp.where(shared, -far[0, :, lanes], 0.0)
        basis[8 * face : 8 * face + 8, lanes] = edge
        edge_out[:, lanes] = edge
        rhs_out[:, lanes] = own[1, :, lanes] - jnp.where(shared, far[1, :, lanes], 0.0)

    row_block = lax.dot_general(
        own[0], basis[...], (((1,), (1,)), ((), ())),
        precision=HIGHEST, preferred_element_type=F32,
    )
    row_block = jnp.where(iota((8, 128), 0) == 6, jnp.broadcast_to(goal_ref[...], (8, 128)), row_block)
    gathered[y, x, z, core] = row_block
    phases = (
        (y, y_send, y_recv, lambda: gathered.at[y, x, z, core], lambda k: at(k, x, z, core)),
        (x, x_send, x_recv, lambda: gathered.at[:, x, z, core], lambda k: at(y, k, z, core)),
        (z, z_send, z_recv, lambda: gathered.at[:, :, z, core], lambda k: at(y, x, k, core)),
    )
    for place, send, recv, part, device in phases:
        copies = [
            remote(part(), part(), send.at[j - 1], recv.at[j - 1], device(turn(place, j)))
            for j in (1, 2, 3)
        ]
        for copy in copies:
            copy.start()
        if place is y:
            top = basis[0:64, :]
            hi = top.astype(BF16)
            basis_out[0:64, :] = hi
            basis_out[64:128, :] = (top - hi.astype(F32)).astype(BF16)
            basis_out[128:192, :] = hi
        for copy in copies:
            copy.wait()
    copy = remote(
        gathered.at[:, :, :, core], gathered.at[:, :, :, core],
        c_send, c_recv, at(y, x, z, 1 - core),
    )
    copy.start()
    copy.wait()
    rows_out[...] = gathered[...].reshape(DEVICES * 8, 128)


def invert_together(blocks, layers):
    lane = iota((8, 128), 1)
    sub = iota((8, 128), 0)

    def node(n, carry):
        base = pl.multiple_of(n * 8, 8)
        results = []
        for layer in layers:
            panel = blocks[layer, pl.ds(base, 8), :]
            cols = [lane_take(panel, jnp.full((8, 128), base + k, jnp.int32)) for k in range(MODES)]
            inside = (lane >> 3) == n
            work = jnp.where(inside, jnp.where(lane - base == sub, 1.0, 0.0), panel)
            for k in range(MODES):
                inv = 1.0 / jnp.broadcast_to(cols[k][k : k + 1, :], (8, 128))
                lift = jnp.where(sub == k, cols[k] - 1.0, cols[k])
                work = work - lift * (jnp.broadcast_to(work[k : k + 1, :], (8, 128)) * inv)
                for j in range(k + 1, MODES):
                    cols[j] = cols[j] - lift * (jnp.broadcast_to(cols[j][k : k + 1, :], (8, 128)) * inv)
            results.append(work)
        for layer, work in zip(layers, results):
            inside = (lane >> 3) == n
            spread = [jnp.broadcast_to(work[k : k + 1, :], (8, 128)) for k in range(MODES)]
            for m in range(16):
                row = blocks[layer, m * 8 : (m + 1) * 8, :]
                out = jnp.where(inside, 0.0, row)
                for k in range(MODES):
                    out = out - lane_take(row, jnp.full((8, 128), base + k, jnp.int32)) * spread[k]
                blocks[layer, m * 8 : (m + 1) * 8, :] = out
            blocks[layer, pl.ds(base, 8), :] = work
        return carry

    lax.fori_loop(0, 16, node, 0)


def mm(a, b):
    return jnp.dot(a, b, precision=HIGHEST, preferred_element_type=F32)


def coarse_kernel(owner, links, place, rows, rows_kept_out, solver_out, blocks, up, down, fold, sel):
    lane = iota((8, 128), 1)
    sub = iota((8, 128), 0)
    offset = owner[0]
    me = place[0]

    def layer_rows(layer, carry):
        for n in range(16):
            slot = (layer * 16 + n + offset) & (DEVICES - 1)
            tile = rows[pl.ds(pl.multiple_of(slot * 8, 8), 8), :]
            real = sub < MODES
            apart = (lane >> 3) - n
            within = lane & 7
            face = jnp.where(apart == 0, 6, jnp.where(apart == -1, 0, jnp.where(
                apart == 1, 1, jnp.where(apart == -4, 2, jnp.where(apart == 4, 3, 7)))))
            linked = (face < 7) & real & (within < MODES)
            block = jnp.where(linked, lane_take(tile, face * 8 + within), 0.0)
            pad = (apart == 0) & (within == sub) & (sub >= MODES)
            blocks[layer, n * 8 : n * 8 + 8, :] = jnp.where(pad, 1.0, block)
            here = (apart == 0) & real & (within < MODES)
            up[layer, n * 8 : n * 8 + 8, :] = jnp.where(here, lane_take(tile, 40 + within), 0.0)
            down[layer, n * 8 : n * 8 + 8, :] = jnp.where(here, lane_take(tile, 32 + within), 0.0)
        return carry

    lax.fori_loop(0, 8, layer_rows, 0)

    own = (me - offset) & (DEVICES - 1)
    for f in range(7):
        target = own if f == 6 else links[0, f]
        for layer in range(8):
            hit = ((lane >> 3) + 16 * layer == target) & ((lane & 7) == sub) & (sub < MODES)
            sel[layer, 8 * f : 8 * f + 8, :] = jnp.where(hit, 1.0, 0.0)
    for layer in range(8):
        sel[layer, 56:64, :] = jnp.zeros((8, 128), F32)

    for k in range(3):
        low, high = k, 7 - k
        invert_together(blocks, (low, high))
        fold[low] = mm(blocks[low], up[low])
        fold[high] = mm(blocks[high], down[high])
        blocks[low + 1] = blocks[low + 1] - mm(down[low + 1], fold[low])
        blocks[high - 1] = blocks[high - 1] - mm(up[high - 1], fold[high])
        sel[low + 1] = sel[low + 1] - mm(sel[low], fold[low])
        sel[high - 1] = sel[high - 1] - mm(sel[high], fold[high])
    invert_together(blocks, (3,))
    fold[3] = mm(blocks[3], up[3])
    blocks[4] = blocks[4] - mm(down[4], fold[3])
    sel[4] = sel[4] - mm(sel[3], fold[3])
    invert_together(blocks, (4,))
    sel[4] = mm(sel[4], blocks[4])
    for k in range(3, -1, -1):
        sel[k] = mm(sel[k] - mm(sel[k + 1], down[k + 1]), blocks[k])
        if k < 3:
            j = 7 - k
            sel[j] = mm(sel[j] - mm(sel[j - 1], up[j - 1]), blocks[j])

    parts = []
    for layer in range(8):
        parts.append(jnp.concatenate(split3(sel[layer]), axis=0).astype(BF16))
    row = iota((128, 128), 0)
    col = iota((128, 128), 1)
    for k in range(MODES):
        total = jnp.zeros((192, 128), F32)
        for layer in range(8):
            slot = ((row >> 3) + 16 * layer + offset) & (DEVICES - 1)
            hot = jnp.where(((row & 7) == k) & (slot == col), 1.0, 0.0).astype(BF16)
            total = total + jnp.dot(parts[layer], hot, preferred_element_type=F32)
        values = total[0:64] + total[64:128] + total[128:192]
        hi = values.astype(BF16)
        solver_out[k * 64 : (k + 1) * 64, 0:128] = hi
        solver_out[k * 64 : (k + 1) * 64, 128:256] = hi
        solver_out[k * 64 : (k + 1) * 64, 256:384] = (values - hi.astype(F32)).astype(BF16)
    rows_kept_out[...] = rows[pl.ds(6, DEVICES, stride=8), :]


def cg_kernel(
    counts, links, map_ref, inverse, modes, edge, rhs, basis, solver, goal, dual_hbm,
    lambda_out, residual_out,
    dual, vec, low_vec, prod, image, far, lam, direction, applied, coarse, live, omega, table,
    dual_sem, halo_send, halo_recv, wide_send, wide_recv,
):
    me = lax.axis_index("dev")
    load = pltpu.make_async_copy(dual_hbm.at[0], dual, dual_sem)
    load.start()
    barrier = pltpu.get_barrier_semaphore()

    def hello(j, carry):
        pl.semaphore_signal(
            barrier, inc=1, device_id=(lax.rem(me + j, DEVICES),), device_id_type=MESH
        )
        return carry

    lax.fori_loop(1, DEVICES, hello, 0)
    pl.semaphore_wait(barrier, DEVICES - 1)

    lane = iota((8, 128), 1)
    sub = iota((8, 128), 0)
    for face in range(FACES):
        spot = iota((8, CAP), 1)
        alive = jnp.where(spot < counts[0, face], 1.0, 0.0)
        limit = jnp.where(links[0, face] >= 0, counts[0, face], 0)
        both = jnp.where(spot < limit, 1.0, 0.0)
        live[:, face_slice(face)] = both
        omega[:, face_slice(face)] = alive - 0.5 * both

    def coarse_solve(even, odd):
        rows = jnp.concatenate([even, odd], axis=1)
        hi = rows.astype(BF16)
        lo = (rows - hi.astype(F32)).astype(BF16)
        out = jnp.dot(
            solver[...], jnp.concatenate([hi, lo, hi], axis=0), preferred_element_type=F32
        )
        total = jnp.zeros((64, 128), F32)
        place = iota((64, 128), 1) & 15
        for k in range(MODES):
            part = out[k * 64 : (k + 1) * 64]
            total = jnp.where(place == k, part[:, :128], total)
            total = jnp.where(place == k + 8, part[:, 128:], total)
        top = total.astype(BF16)
        rest = (total - top.astype(F32)).astype(BF16)
        pair = jnp.concatenate([top, rest], axis=1)
        triple = jnp.concatenate([pair, pair, pair], axis=0)
        group = jnp.where(
            ((iota((8, 256), 1) & 127) >> 4) == iota((8, 256), 0), 1.0, 0.0
        ).astype(BF16)
        return lax.dot_general(
            group, triple, (((1,), (1,)), ((), ())), preferred_element_type=F32
        )

    def expand(z3):
        top = z3.astype(BF16).astype(F32)
        packed = jnp.where(iota((8, 192), 1) < 128, top, z3 - top).astype(BF16)
        return jnp.dot(packed, basis[...], preferred_element_type=F32)

    def halo(parity):
        return [
            remote(
                image.at[:, face_slice(face)], far.at[parity, :, face_slice(OPPOSITE[face])],
                halo_send.at[parity, face], halo_recv.at[parity, OPPOSITE[face]],
                neighbour(me, FACE_STEPS[face]),
            )
            for face in range(FACES)
        ]

    def dual_apply(parity):
        def to_columns(o, carry):
            lanes = pl.ds(pl.multiple_of(o * 128, 128), 128)
            low_vec[:, lanes] = permuted_chunk(vec, map_ref[:, lanes]).astype(BF16)
            return carry

        lax.fori_loop(0, CHUNKS, to_columns, 0)

        def product(n, carry):
            lanes = pl.ds(pl.multiple_of(n * 512, 512), 512)
            prod[:, lanes] = jnp.dot(low_vec[...], dual[:, lanes], preferred_element_type=F32)
            return carry

        lax.fori_loop(0, NMAX // 512, product, 0)

        def to_faces(r, carry):
            lanes = pl.ds(pl.multiple_of(r * 128, 128), 128)
            piece = permuted_chunk(prod, inverse[pl.ds(r, 1), :])
            image[:, lanes] = jnp.where(omega[:, lanes] > 0.0, piece, 0.0)
            return carry

        lax.fori_loop(0, CHUNKS, to_faces, 0)
        for copy in halo(parity):
            copy.start()

    def assembled(parity):
        for copy in halo(parity):
            copy.wait()
        return image[...] - live[...] * far[parity]

    def slot_rows(slot):
        return pl.ds(pl.multiple_of(slot * 4, 4), 4)

    def share(parity, own, faces, extra):
        tiles = []
        for r in range(4):
            columns = list(enumerate(own)) + [(6 + k, e) for k, e in enumerate(extra)]
            if r > 0:
                columns = list(enumerate(faces[2 * r - 2]))
                columns += [(8 + k, e) for k, e in enumerate(faces[2 * r - 1])]
            tile = jnp.zeros((8, 128), F32)
            for k, values in columns:
                tile = jnp.where((lane & 15) == k, values, tile)
            tiles.append(jnp.sum(jnp.where((lane >> 4) == sub, tile, 0.0), axis=0, keepdims=True))
        table[parity, slot_rows(me), :] = jnp.concatenate(tiles, axis=0)

        def send(j, carry):
            part = table.at[parity, slot_rows(me), :]
            remote(
                part, part, wide_send.at[parity], wide_recv.at[parity], lax.rem(me + j, DEVICES)
            ).start()
            return carry

        lax.fori_loop(1, DEVICES, send, 0)
        most = table.at[parity, pl.ds(0, 4 * DEVICES - 4), :]
        everything = remote(
            most, most, wide_send.at[parity], wide_recv.at[parity], lax.rem(me + 1, DEVICES)
        )
        everything.wait()
        first = table[parity, pl.ds(0, DEVICES, stride=4), :]
        even, odd = first, jnp.zeros((DEVICES, 128), F32)
        for r in range(3):
            pair = table[parity, pl.ds(r + 1, DEVICES, stride=4), :]
            even = even + pltpu.roll(pair, FACE_STEPS[2 * r] % DEVICES, 0)
            odd = odd + pltpu.roll(pair, FACE_STEPS[2 * r + 1] % DEVICES, 0)
        return first, even, odd

    def mode_sums(values):
        return [
            jnp.sum(modes[a : a + 1, :] * values, axis=1, keepdims=True) for a in range(MODES)
        ]

    def face_sums(values):
        return [
            [
                jnp.sum(
                    edge[a : a + 1, face * CAP : (face + 1) * CAP]
                    * values[:, face * CAP : (face + 1) * CAP],
                    axis=1, keepdims=True,
                )
                for a in range(MODES)
            ]
            for face in range(FACES)
        ]

    def summed(product):
        return jnp.sum(product, axis=1, keepdims=True)

    def total_of(totals, k):
        return jnp.sum(jnp.where(lane == 16 * sub + k, totals, 0.0), axis=1, keepdims=True)

    start = expand(coarse_solve(goal[...], jnp.zeros((DEVICES, 128), F32)))
    lam[...] = start
    vec[...] = start
    load.wait()
    dual_apply(0)
    negative = -image[...]
    _, even, odd = share(0, mode_sums(rhs[...] + negative), face_sums(negative), [])
    z3 = coarse_solve(even, odd)
    vec[...] = rhs[...] - assembled(0) - expand(z3)
    direction[...] = jnp.zeros_like(direction)
    applied[...] = jnp.zeros_like(applied)
    coarse[...] = jnp.zeros_like(coarse)

    def iteration(step, carry):
        rho_old, curve_old = carry
        parity = lax.rem(step, 2)
        dual_apply(parity)
        w = vec[...]
        y = image[...]
        extra = [
            summed(omega[...] * w * w), summed(w * y), summed(omega[...] * w * applied[...]),
            summed(direction[...] * y),
        ]
        first, even, odd = share(parity, mode_sums(y), face_sums(y), extra)
        totals = jnp.broadcast_to(jnp.sum(first, axis=0, keepdims=True), (8, 128))
        rho = total_of(totals, 6)
        ratio = rho / rho_old
        curve = (
            total_of(totals, 7) + ratio * (total_of(totals, 8) + total_of(totals, 9))
            + ratio * ratio * curve_old
        )
        length = rho / curve
        z3 = coarse_solve(even, odd) + ratio * coarse[...]
        coarse[...] = z3
        image_of = assembled(parity) + ratio * applied[...]
        applied[...] = image_of
        way = vec[...] + ratio * direction[...]
        direction[...] = way
        lam[...] = lam[...] + length * way
        vec[...] = vec[...] - length * (image_of - expand(z3))
        return rho, curve

    far_off = jnp.full((8, 1), jnp.inf, F32)
    lax.fori_loop(1, ITERS + 1, iteration, (far_off, jnp.zeros((8, 1), F32)))

    def to_outputs(o, carry):
        lanes = pl.ds(pl.multiple_of(o * 128, 128), 128)
        row = map_ref[:, lanes]
        lambda_out[0, :, lanes] = permuted_chunk(lam, row)
        residual_out[0, :, lanes] = permuted_chunk(vec, row)
        return carry

    lax.fori_loop(0, CHUNKS, to_outputs, 0)


VM = pl.BlockSpec(memory_space=pltpu.VMEM)
SM = pl.BlockSpec(memory_space=pltpu.SMEM)
DMA = pltpu.SemaphoreType.DMA


def sds(shape, dtype=F32):
    return jax.ShapeDtypeStruct(shape, dtype)


def per_device(
    dual_blocks, rigid_modes, dual_local, coarse_rhs,
    iface_sizes, neighbours, shared_counts, iface_map, owner,
):
    goal_row = jnp.pad(coarse_rhs[0].T, ((0, 0), (0, 16 - MODES))).reshape(1, 128)
    rows, basis, modes, edge, rhs, inverse = pl.pallas_call(
        setup_kernel,
        out_shape=(
            sds((DEVICES * 8, 128)), sds((192, NMAX), BF16), sds((8, NMAX)), sds((8, NMAX)),
            sds((8, NMAX)), sds((CHUNKS, 128), jnp.int32),
        ),
        in_specs=[SM, SM, VM, VM, VM, VM],
        out_specs=(VM,) * 6,
        scratch_shapes=[
            pltpu.VMEM((8, NMAX), F32), pltpu.VMEM((2, 8, NMAX), F32),
            pltpu.VMEM((2, 8, NMAX), F32), pltpu.VMEM((128, NMAX), F32),
            pltpu.VMEM((4, 4, 4, 2, 8, 128), F32),
            DMA((6,)), DMA((6,)), DMA((3,)), DMA((3,)), DMA((3,)), DMA((3,)),
            DMA((3,)), DMA((3,)), DMA, DMA,
        ],
        compiler_params=pltpu.CompilerParams(
            collective_id=0, has_side_effects=True, vmem_limit_bytes=40 << 20
        ),
        name="setup",
    )(shared_counts, neighbours, iface_map, rigid_modes, dual_local, goal_row)

    place = lax.axis_index("dev").astype(jnp.int32).reshape(1)
    goal, solver = pl.pallas_call(
        coarse_kernel,
        out_shape=(sds((DEVICES, 128)), sds((64 * MODES, 384), BF16)),
        in_specs=[SM, SM, SM, VM],
        out_specs=(VM, VM),
        scratch_shapes=[
            pltpu.VMEM((8, 128, 128), F32), pltpu.VMEM((8, 128, 128), F32),
            pltpu.VMEM((8, 128, 128), F32), pltpu.VMEM((8, 128, 128), F32),
            pltpu.VMEM((8, 64, 128), F32),
        ],
        compiler_params=pltpu.CompilerParams(vmem_limit_bytes=40 << 20),
        name="coarse",
    )(owner, neighbours, place, rows)

    return pl.pallas_call(
        cg_kernel,
        out_shape=(sds((1, LOADS, NMAX)), sds((1, LOADS, NMAX))),
        in_specs=[SM, SM] + [VM] * 8 + [pl.BlockSpec(memory_space=pl.ANY)],
        out_specs=(VM, VM),
        scratch_shapes=[
            pltpu.VMEM((NMAX, NMAX), BF16), pltpu.VMEM((8, NMAX), F32),
            pltpu.VMEM((8, NMAX), BF16),
        ] + [pltpu.VMEM((8, NMAX), F32)] * 2 + [pltpu.VMEM((2, 8, NMAX), F32)]
        + [pltpu.VMEM((8, NMAX), F32)] * 3 + [
            pltpu.VMEM((8, 192), F32), pltpu.VMEM((8, NMAX), F32), pltpu.VMEM((8, NMAX), F32),
            pltpu.VMEM((2, 4 * DEVICES, 128), F32),
            DMA, DMA((2, 6)), DMA((2, 6)), DMA((2,)), DMA((2,)),
        ],
        compiler_params=pltpu.CompilerParams(
            collective_id=1, has_side_effects=True, vmem_limit_bytes=56 << 20
        ),
        name="gradients",
    )(
        shared_counts, neighbours, iface_map, inverse, modes, edge, rhs, basis, solver, goal,
        dual_blocks,
    )


def solution(mesh):
    in_specs = (
        P("dev", None, None), P("dev", None, None), P("dev", None, None), P("dev", None, None),
        P("dev"), P("dev", None), P("dev", None), P("dev", None), P(),
    )
    out_specs = (P("dev", None, None), P("dev", None, None))
    return jax.shard_map(
        per_device, mesh=mesh, in_specs=in_specs, out_specs=out_specs, check_vma=False
    )
```

```python
import functools

import jax
import jax.numpy as jnp
from jax import lax
from jax.experimental import pallas as pl
from jax.experimental.pallas import tpu as pltpu
from jax.sharding import PartitionSpec as P

FACES = 6
MODES = 6
CAP = 512
NMAX = 3072
LOADS = 8
CHUNKS = NMAX // 128
ITERS = 3
GROUP = 4
DEVICES = 128
OPPOSITE = (1, 0, 3, 2, 5, 4)
FACE_STEPS = (-1, 1, -4, 4, -16, 16)
HIGHEST = lax.Precision.HIGHEST
F32 = jnp.float32
BF16 = jnp.bfloat16
MESH = pl.DeviceIdType.MESH


def iota(shape, dim):
    return lax.broadcasted_iota(jnp.int32, shape, dim)


def lane_take(values, lanes):
    return jnp.take_along_axis(values, lanes, axis=1, mode="promise_in_bounds")


def permuted_chunk(src, index_row):
    index = jnp.broadcast_to(index_row, (8, 128))
    chunk = index >> 7
    lanes = index & 127
    out = jnp.zeros((8, 128), F32)
    for s in range(CHUNKS):
        piece = lane_take(src[:, s * 128 : (s + 1) * 128], lanes)
        out = jnp.where(chunk == s, piece, out)
    return out


def neighbour(me, step):
    return lax.rem(me + step + DEVICES, DEVICES)


def face_slice(face):
    return pl.ds(face * CAP, CAP)


def greet_all(me):
    barrier = pltpu.get_barrier_semaphore()

    def hello(j, carry):
        pl.semaphore_signal(
            barrier, inc=1, device_id=(lax.rem(me + j, DEVICES),), device_id_type=MESH
        )
        return carry

    lax.fori_loop(1, DEVICES, hello, 0)
    pl.semaphore_wait(barrier, DEVICES - 1)


def remote(src, dst, send, recv, device):
    return pltpu.make_async_remote_copy(
        src_ref=src, dst_ref=dst, send_sem=send, recv_sem=recv,
        device_id=(device,), device_id_type=MESH,
    )


def split3(x):
    hi = x.astype(BF16).astype(F32)
    rest = x - hi
    mid = rest.astype(BF16).astype(F32)
    return hi, mid, rest - mid


def setup_kernel(
    counts, links, map_ref, modes_ref, rhs_ref, goal_ref,
    rows_out, basis_out, modes_out, edge_out, rhs_out, inverse_out,
    padded, own, far, basis, gathered, halo_send, halo_recv, wide_send, wide_recv,
):
    me = lax.axis_index("dev")
    greet_all(me)

    codes = map_ref[...]
    high = jnp.where(codes >= 0, codes >> 7, -1)
    low = jnp.where(codes >= 0, codes & 127, -1)
    column = iota((32, NMAX), 1)
    here = jnp.broadcast_to(high, (32, NMAX)) == iota((32, NMAX), 0)
    coarse_digit = jnp.where(here, column >> 6, 0).astype(F32).astype(BF16)
    fine_digit = jnp.where(here, column & 63, 0).astype(F32).astype(BF16)
    spots = (
        jnp.broadcast_to(low, (128, NMAX)) == iota((128, NMAX), 0)
    ).astype(F32).astype(BF16)
    digits = lax.dot_general(
        jnp.concatenate([coarse_digit, fine_digit], axis=0), spots,
        (((1,), (1,)), ((), ())), preferred_element_type=F32,
    )
    inverse = (digits[:32] * 64.0 + digits[32:]).astype(jnp.int32)
    inverse_out[...] = inverse[:CHUNKS]

    padded[...] = jnp.zeros_like(padded)
    padded[0:MODES, :] = modes_ref[0]
    for r in range(CHUNKS):
        face = r // 4
        live = iota((8, 128), 1) + (r % 4) * 128 < counts[0, face]
        row = inverse_out[r : r + 1, :]
        own[0, :, r * 128 : (r + 1) * 128] = jnp.where(live, permuted_chunk(padded, row), 0.0)
        own[1, :, r * 128 : (r + 1) * 128] = jnp.where(live, permuted_chunk(rhs_ref.at[0], row), 0.0)

    copies = [
        remote(
            own.at[:, :, face_slice(face)], far.at[:, :, face_slice(OPPOSITE[face])],
            halo_send.at[face], halo_recv.at[OPPOSITE[face]], neighbour(me, FACE_STEPS[face]),
        )
        for face in range(FACES)
    ]
    for copy in copies:
        copy.start()
    basis[...] = jnp.zeros_like(basis)
    basis[48:56, :] = own[0]
    modes_out[...] = own[0]
    for copy in copies:
        copy.wait()
    for face in range(FACES):
        limit = jnp.where(links[0, face] >= 0, counts[0, face], 0)
        shared = iota((8, CAP), 1) < limit
        lanes = face_slice(face)
        edge = jnp.where(shared, -far[0, :, lanes], 0.0)
        basis[8 * face : 8 * face + 8, lanes] = edge
        edge_out[:, lanes] = edge
        rhs_out[:, lanes] = own[1, :, lanes] - jnp.where(shared, far[1, :, lanes], 0.0)

    row_block = lax.dot_general(
        own[0], basis[...], (((1,), (1,)), ((), ())),
        precision=HIGHEST, preferred_element_type=F32,
    )
    row_block = jnp.where(iota((8, 128), 0) == 6, jnp.broadcast_to(goal_ref[...], (8, 128)), row_block)
    mine = pl.ds(pl.multiple_of(me * 8, 8), 8)
    gathered[mine, :] = row_block

    def send(j, carry):
        part = gathered.at[mine, :]
        remote(part, part, wide_send, wide_recv, lax.rem(me + j, DEVICES)).start()
        return carry

    lax.fori_loop(1, DEVICES, send, 0)
    top = basis[0:64, :]
    hi = top.astype(BF16)
    basis_out[0:64, :] = hi
    basis_out[64:128, :] = (top - hi.astype(F32)).astype(BF16)
    basis_out[128:192, :] = hi
    most = gathered.at[pl.ds(0, 8 * DEVICES - 8), :]
    remote(most, most, wide_send, wide_recv, lax.rem(me + 1, DEVICES)).wait()
    rows_out[...] = gathered[...]


def invert_together(blocks, layers):
    lane = iota((8, 128), 1)
    sub = iota((8, 128), 0)

    def spread(values, k):
        return jnp.broadcast_to(values[k : k + 1, :], (8, 128))

    def pair(n, carry):
        base = pl.multiple_of(n * 16, 16)
        pivots = [(half, k) for half in range(2) for k in range(MODES)]
        picks = [jnp.full((8, 128), base + 8 * half + k, jnp.int32) for half, k in pivots]
        group = lane >> 4
        inside = group == n
        panels = [
            [blocks[layer, pl.ds(base + 8 * half, 8), :] for half in range(2)] for layer in layers
        ]
        results = []
        for panel in panels:
            cols = [[lane_take(part, pick) for part in panel] for pick in picks]
            work = [
                jnp.where(inside, jnp.where(lane - base == sub + 8 * half, 1.0, 0.0), panel[half])
                for half in range(2)
            ]
            for p, (half, k) in enumerate(pivots):
                inv = 1.0 / spread(cols[p][half], k)
                lift = list(cols[p])
                lift[half] = jnp.where(sub == k, lift[half] - 1.0, lift[half])
                lift = [part * inv for part in lift]
                for target in [work] + cols[p + 1 :]:
                    row = spread(target[half], k)
                    for other in range(2):
                        target[other] = target[other] - lift[other] * row
            results.append(jnp.concatenate(work, axis=0))
        for layer, panel, work in zip(layers, panels, results):
            column = jnp.concatenate([jnp.where(group < n, -part, part) for part in panel], axis=0)
            a, b, c = split3(column)
            d, e, f = split3(work)
            left = jnp.concatenate([a, a, b, a, c, b], axis=0).astype(BF16)
            right = jnp.concatenate([d, e, d, f, d, e], axis=0).astype(BF16)
            change = lax.dot_general(
                left, right, (((0,), (0,)), ((), ())), preferred_element_type=F32
            )
            clear = (iota((128, 128), 1) >> 4) == n
            blocks[layer] = jnp.where(clear, 0.0, blocks[layer]) - change
            blocks[layer, pl.ds(base, 16), :] = work
        return carry

    lax.fori_loop(0, 8, pair, 0)


def mm(a, b):
    return jnp.dot(a, b, precision=HIGHEST, preferred_element_type=F32)


def coarse_kernel(owner, links, place, rows, rows_kept_out, solver_out, blocks, up, down, fold, sel):
    lane = iota((8, 128), 1)
    sub = iota((8, 128), 0)
    offset = owner[0]
    me = place[0]

    def layer_rows(layer, carry):
        for n in range(16):
            slot = (layer * 16 + n + offset) & (DEVICES - 1)
            tile = rows[pl.ds(pl.multiple_of(slot * 8, 8), 8), :]
            real = sub < MODES
            apart = (lane >> 3) - n
            within = lane & 7
            face = jnp.where(apart == 0, 6, jnp.where(apart == -1, 0, jnp.where(
                apart == 1, 1, jnp.where(apart == -4, 2, jnp.where(apart == 4, 3, 7)))))
            linked = (face < 7) & real & (within < MODES)
            block = jnp.where(linked, lane_take(tile, face * 8 + within), 0.0)
            pad = (apart == 0) & (within == sub) & (sub >= MODES)
            blocks[layer, n * 8 : n * 8 + 8, :] = jnp.where(pad, 1.0, block)
            here = (apart == 0) & real & (within < MODES)
            up[layer, n * 8 : n * 8 + 8, :] = jnp.where(here, lane_take(tile, 40 + within), 0.0)
            down[layer, n * 8 : n * 8 + 8, :] = jnp.where(here, lane_take(tile, 32 + within), 0.0)
        return carry

    lax.fori_loop(0, 8, layer_rows, 0)

    own = (me - offset) & (DEVICES - 1)
    for f in range(7):
        target = own if f == 6 else links[0, f]
        for layer in range(8):
            hit = ((lane >> 3) + 16 * layer == target) & ((lane & 7) == sub) & (sub < MODES)
            sel[layer, 8 * f : 8 * f + 8, :] = jnp.where(hit, 1.0, 0.0)
    for layer in range(8):
        sel[layer, 56:64, :] = jnp.zeros((8, 128), F32)

    for k in range(3):
        low, high = k, 7 - k
        invert_together(blocks, (low, high))
        fold[low] = mm(blocks[low], up[low])
        fold[high] = mm(blocks[high], down[high])
        blocks[low + 1] = blocks[low + 1] - mm(down[low + 1], fold[low])
        blocks[high - 1] = blocks[high - 1] - mm(up[high - 1], fold[high])
        sel[low + 1] = sel[low + 1] - mm(sel[low], fold[low])
        sel[high - 1] = sel[high - 1] - mm(sel[high], fold[high])
    invert_together(blocks, (3,))
    fold[3] = mm(blocks[3], up[3])
    blocks[4] = blocks[4] - mm(down[4], fold[3])
    sel[4] = sel[4] - mm(sel[3], fold[3])
    invert_together(blocks, (4,))
    sel[4] = mm(sel[4], blocks[4])
    for k in range(3, -1, -1):
        sel[k] = mm(sel[k] - mm(sel[k + 1], down[k + 1]), blocks[k])
        if k < 3:
            j = 7 - k
            sel[j] = mm(sel[j] - mm(sel[j - 1], up[j - 1]), blocks[j])

    parts = []
    for layer in range(8):
        parts.append(jnp.concatenate(split3(sel[layer]), axis=0).astype(BF16))
    row = iota((128, 128), 0)
    col = iota((128, 128), 1)
    for k in range(MODES):
        total = jnp.zeros((192, 128), F32)
        for layer in range(8):
            slot = ((row >> 3) + 16 * layer + offset) & (DEVICES - 1)
            hot = jnp.where(((row & 7) == k) & (slot == col), 1.0, 0.0).astype(BF16)
            total = total + jnp.dot(parts[layer], hot, preferred_element_type=F32)
        values = total[0:64] + total[64:128] + total[128:192]
        hi = values.astype(BF16)
        solver_out[k * 64 : (k + 1) * 64, 0:128] = hi
        solver_out[k * 64 : (k + 1) * 64, 128:256] = hi
        solver_out[k * 64 : (k + 1) * 64, 256:384] = (values - hi.astype(F32)).astype(BF16)
    rows_kept_out[...] = rows[pl.ds(6, DEVICES, stride=8), :]


def cg_kernel(
    counts, links, map_ref, inverse, modes, edge, rhs, basis, solver, goal, dual_hbm,
    lambda_out, residual_out,
    dual, vec, low_vec, prod, image, far, lam, direction, applied, coarse, live, omega, table,
    dual_sem, halo_send, halo_recv, wide_send, wide_recv,
):
    me = lax.axis_index("dev")
    load = pltpu.make_async_copy(dual_hbm.at[0], dual, dual_sem)
    load.start()
    greet_all(me)

    lane = iota((8, 128), 1)
    sub = iota((8, 128), 0)
    for face in range(FACES):
        spot = iota((8, CAP), 1)
        alive = jnp.where(spot < counts[0, face], 1.0, 0.0)
        limit = jnp.where(links[0, face] >= 0, counts[0, face], 0)
        both = jnp.where(spot < limit, 1.0, 0.0)
        live[:, face_slice(face)] = both
        omega[:, face_slice(face)] = alive - 0.5 * both

    def coarse_solve(even, odd):
        rows = jnp.concatenate([even, odd], axis=1)
        hi = rows.astype(BF16)
        lo = (rows - hi.astype(F32)).astype(BF16)
        out = jnp.dot(
            solver[...], jnp.concatenate([hi, lo, hi], axis=0), preferred_element_type=F32
        )
        total = jnp.zeros((64, 128), F32)
        place = iota((64, 128), 1) & 15
        for k in range(MODES):
            part = out[k * 64 : (k + 1) * 64]
            total = jnp.where(place == k, part[:, :128], total)
            total = jnp.where(place == k + 8, part[:, 128:], total)
        top = total.astype(BF16)
        rest = (total - top.astype(F32)).astype(BF16)
        pair = jnp.concatenate([top, rest], axis=1)
        triple = jnp.concatenate([pair, pair, pair], axis=0)
        group = jnp.where(
            ((iota((8, 256), 1) & 127) >> 4) == iota((8, 256), 0), 1.0, 0.0
        ).astype(BF16)
        return lax.dot_general(
            group, triple, (((1,), (1,)), ((), ())), preferred_element_type=F32
        )

    def expand(z3):
        top = z3.astype(BF16).astype(F32)
        packed = jnp.where(iota((8, 192), 1) < 128, top, z3 - top).astype(BF16)
        return jnp.dot(packed, basis[...], preferred_element_type=F32)

    def halo(parity):
        return [
            remote(
                image.at[:, face_slice(face)], far.at[parity, :, face_slice(OPPOSITE[face])],
                halo_send.at[parity, face], halo_recv.at[parity, OPPOSITE[face]],
                neighbour(me, FACE_STEPS[face]),
            )
            for face in range(FACES)
        ]

    def dual_apply(parity):
        def to_columns(o, carry):
            for g in range(GROUP):
                lanes = pl.ds(pl.multiple_of((o * GROUP + g) * 128, 128), 128)
                low_vec[:, lanes] = permuted_chunk(vec, map_ref[:, lanes]).astype(BF16)
            return carry

        lax.fori_loop(0, CHUNKS // GROUP, to_columns, 0)

        def product(n, carry):
            lanes = pl.ds(pl.multiple_of(n * 512, 512), 512)
            prod[:, lanes] = jnp.dot(low_vec[...], dual[:, lanes], preferred_element_type=F32)
            return carry

        lax.fori_loop(0, NMAX // 512, product, 0)

        def to_faces(o, carry):
            for g in range(GROUP):
                r = o * GROUP + g
                lanes = pl.ds(pl.multiple_of(r * 128, 128), 128)
                piece = permuted_chunk(prod, inverse[pl.ds(r, 1), :])
                image[:, lanes] = jnp.where(omega[:, lanes] > 0.0, piece, 0.0)
            return carry

        lax.fori_loop(0, CHUNKS // GROUP, to_faces, 0)
        for copy in halo(parity):
            copy.start()

    def assembled(parity):
        for copy in halo(parity):
            copy.wait()
        return image[...] - live[...] * far[parity]

    def slot_rows(slot):
        return pl.ds(pl.multiple_of(slot * 4, 4), 4)

    def share(parity, own, faces, extra):
        tiles = []
        for r in range(4):
            columns = list(enumerate(own)) + [(6 + k, e) for k, e in enumerate(extra)]
            if r > 0:
                columns = list(enumerate(faces[2 * r - 2]))
                columns += [(8 + k, e) for k, e in enumerate(faces[2 * r - 1])]
            tile = jnp.zeros((8, 128), F32)
            for k, values in columns:
                tile = jnp.where((lane & 15) == k, values, tile)
            tiles.append(jnp.sum(jnp.where((lane >> 4) == sub, tile, 0.0), axis=0, keepdims=True))
        table[parity, slot_rows(me), :] = jnp.concatenate(tiles, axis=0)

        def send(j, carry):
            part = table.at[parity, slot_rows(me), :]
            remote(
                part, part, wide_send.at[parity], wide_recv.at[parity], lax.rem(me + j, DEVICES)
            ).start()
            return carry

        lax.fori_loop(1, DEVICES, send, 0)
        most = table.at[parity, pl.ds(0, 4 * DEVICES - 4), :]
        everything = remote(
            most, most, wide_send.at[parity], wide_recv.at[parity], lax.rem(me + 1, DEVICES)
        )
        everything.wait()
        first = table[parity, pl.ds(0, DEVICES, stride=4), :]
        even, odd = first, jnp.zeros((DEVICES, 128), F32)
        for r in range(3):
            pair = table[parity, pl.ds(r + 1, DEVICES, stride=4), :]
            even = even + pltpu.roll(pair, FACE_STEPS[2 * r] % DEVICES, 0)
            odd = odd + pltpu.roll(pair, FACE_STEPS[2 * r + 1] % DEVICES, 0)
        return first, even, odd

    def mode_sums(values):
        return [
            jnp.sum(modes[a : a + 1, :] * values, axis=1, keepdims=True) for a in range(MODES)
        ]

    def face_sums(values):
        return [
            [
                jnp.sum(
                    edge[a : a + 1, face * CAP : (face + 1) * CAP]
                    * values[:, face * CAP : (face + 1) * CAP],
                    axis=1, keepdims=True,
                )
                for a in range(MODES)
            ]
            for face in range(FACES)
        ]

    def summed(product):
        return jnp.sum(product, axis=1, keepdims=True)

    def total_of(totals, k):
        return jnp.sum(jnp.where(lane == 16 * sub + k, totals, 0.0), axis=1, keepdims=True)

    start = expand(coarse_solve(goal[...], jnp.zeros((DEVICES, 128), F32)))
    lam[...] = start
    vec[...] = start
    load.wait()
    dual_apply(0)
    negative = -image[...]
    _, even, odd = share(0, mode_sums(rhs[...] + negative), face_sums(negative), [])
    z3 = coarse_solve(even, odd)
    vec[...] = rhs[...] - assembled(0) - expand(z3)
    direction[...] = jnp.zeros_like(direction)
    applied[...] = jnp.zeros_like(applied)
    coarse[...] = jnp.zeros_like(coarse)

    def iteration(step, carry):
        rho_old, curve_old = carry
        parity = lax.rem(step, 2)
        dual_apply(parity)
        w = vec[...]
        y = image[...]
        extra = [
            summed(omega[...] * w * w), summed(w * y), summed(omega[...] * w * applied[...]),
            summed(direction[...] * y),
        ]
        first, even, odd = share(parity, mode_sums(y), face_sums(y), extra)
        totals = jnp.broadcast_to(jnp.sum(first, axis=0, keepdims=True), (8, 128))
        rho = total_of(totals, 6)
        ratio = rho / rho_old
        curve = (
            total_of(totals, 7) + ratio * (total_of(totals, 8) + total_of(totals, 9))
            + ratio * ratio * curve_old
        )
        length = rho / curve
        z3 = coarse_solve(even, odd) + ratio * coarse[...]
        coarse[...] = z3
        image_of = assembled(parity) + ratio * applied[...]
        applied[...] = image_of
        way = vec[...] + ratio * direction[...]
        direction[...] = way
        lam[...] = lam[...] + length * way
        vec[...] = vec[...] - length * (image_of - expand(z3))
        return rho, curve

    far_off = jnp.full((8, 1), jnp.inf, F32)
    lax.fori_loop(1, ITERS + 1, iteration, (far_off, jnp.zeros((8, 1), F32)))

    def to_outputs(o, carry):
        for g in range(GROUP):
            lanes = pl.ds(pl.multiple_of((o * GROUP + g) * 128, 128), 128)
            row = map_ref[:, lanes]
            lambda_out[0, :, lanes] = permuted_chunk(lam, row)
            residual_out[0, :, lanes] = permuted_chunk(vec, row)
        return carry

    lax.fori_loop(0, CHUNKS // GROUP, to_outputs, 0)


VM = pl.BlockSpec(memory_space=pltpu.VMEM)
SM = pl.BlockSpec(memory_space=pltpu.SMEM)
DMA = pltpu.SemaphoreType.DMA


def sds(shape, dtype=F32):
    return jax.ShapeDtypeStruct(shape, dtype)


def per_device(
    dual_blocks, rigid_modes, dual_local, coarse_rhs,
    iface_sizes, neighbours, shared_counts, iface_map, owner,
):
    goal_row = jnp.pad(coarse_rhs[0].T, ((0, 0), (0, 16 - MODES))).reshape(1, 128)
    rows, basis, modes, edge, rhs, inverse = pl.pallas_call(
        setup_kernel,
        out_shape=(
            sds((DEVICES * 8, 128)), sds((192, NMAX), BF16), sds((8, NMAX)), sds((8, NMAX)),
            sds((8, NMAX)), sds((CHUNKS, 128), jnp.int32),
        ),
        in_specs=[SM, SM, VM, VM, VM, VM],
        out_specs=(VM,) * 6,
        scratch_shapes=[
            pltpu.VMEM((8, NMAX), F32), pltpu.VMEM((2, 8, NMAX), F32),
            pltpu.VMEM((2, 8, NMAX), F32), pltpu.VMEM((128, NMAX), F32),
            pltpu.VMEM((DEVICES * 8, 128), F32), DMA((6,)), DMA((6,)), DMA, DMA,
        ],
        compiler_params=pltpu.CompilerParams(
            collective_id=0, has_side_effects=True, vmem_limit_bytes=40 << 20
        ),
        name="setup",
    )(shared_counts, neighbours, iface_map, rigid_modes, dual_local, goal_row)

    place = lax.axis_index("dev").astype(jnp.int32).reshape(1)
    goal, solver = pl.pallas_call(
        coarse_kernel,
        out_shape=(sds((DEVICES, 128)), sds((64 * MODES, 384), BF16)),
        in_specs=[SM, SM, SM, VM],
        out_specs=(VM, VM),
        scratch_shapes=[
            pltpu.VMEM((8, 128, 128), F32), pltpu.VMEM((8, 128, 128), F32),
            pltpu.VMEM((8, 128, 128), F32), pltpu.VMEM((8, 128, 128), F32),
            pltpu.VMEM((8, 64, 128), F32),
        ],
        compiler_params=pltpu.CompilerParams(vmem_limit_bytes=40 << 20),
        name="coarse",
    )(owner, neighbours, place, rows)

    return pl.pallas_call(
        cg_kernel,
        out_shape=(sds((1, LOADS, NMAX)), sds((1, LOADS, NMAX))),
        in_specs=[SM, SM] + [VM] * 8 + [pl.BlockSpec(memory_space=pl.ANY)],
        out_specs=(VM, VM),
        scratch_shapes=[
            pltpu.VMEM((NMAX, NMAX), BF16), pltpu.VMEM((8, NMAX), F32),
            pltpu.VMEM((8, NMAX), BF16),
        ] + [pltpu.VMEM((8, NMAX), F32)] * 2 + [pltpu.VMEM((2, 8, NMAX), F32)]
        + [pltpu.VMEM((8, NMAX), F32)] * 3 + [
            pltpu.VMEM((8, 192), F32), pltpu.VMEM((8, NMAX), F32), pltpu.VMEM((8, NMAX), F32),
            pltpu.VMEM((2, 4 * DEVICES, 128), F32),
            DMA, DMA((2, 6)), DMA((2, 6)), DMA((2,)), DMA((2,)),
        ],
        compiler_params=pltpu.CompilerParams(
            collective_id=1, has_side_effects=True, vmem_limit_bytes=56 << 20
        ),
        name="gradients",
    )(
        shared_counts, neighbours, iface_map, inverse, modes, edge, rhs, basis, solver, goal,
        dual_blocks,
    )


def solution(mesh):
    in_specs = (
        P("dev", None, None), P("dev", None, None), P("dev", None, None), P("dev", None, None),
        P("dev"), P("dev", None), P("dev", None), P("dev", None), P(),
    )
    out_specs = (P("dev", None, None), P("dev", None, None))
    return jax.shard_map(
        per_device, mesh=mesh, in_specs=in_specs, out_specs=out_specs, check_vma=False
    )
```

```python
import functools

import jax
import jax.numpy as jnp
from jax import lax
from jax.experimental import pallas as pl
from jax.experimental.pallas import tpu as pltpu
from jax.sharding import PartitionSpec as P

FACES = 6
MODES = 6
CAP = 512
NMAX = 3072
LOADS = 8
CHUNKS = NMAX // 128
ITERS = 3
GROUP = 8
DEVICES = 128
OPPOSITE = (1, 0, 3, 2, 5, 4)
FACE_STEPS = (-1, 1, -4, 4, -16, 16)
HIGHEST = lax.Precision.HIGHEST
F32 = jnp.float32
BF16 = jnp.bfloat16
MESH = pl.DeviceIdType.MESH


def iota(shape, dim):
    return lax.broadcasted_iota(jnp.int32, shape, dim)


def lane_take(values, lanes):
    return jnp.take_along_axis(values, lanes, axis=1, mode="promise_in_bounds")


def permuted_chunk(src, index_row):
    index = jnp.broadcast_to(index_row, (8, 128))
    chunk = index >> 7
    lanes = index & 127
    out = jnp.zeros((8, 128), F32)
    for s in range(CHUNKS):
        piece = lane_take(src[:, s * 128 : (s + 1) * 128], lanes)
        out = jnp.where(chunk == s, piece, out)
    return out


def neighbour(me, step):
    return lax.rem(me + step + DEVICES, DEVICES)


def face_slice(face):
    return pl.ds(face * CAP, CAP)


def greet_all(me):
    barrier = pltpu.get_barrier_semaphore()

    to_everyone(me, lambda device: pl.semaphore_signal(
        barrier, inc=1, device_id=(device,), device_id_type=MESH
    ))


def slot_rows(slot):
    return pl.ds(pl.multiple_of(slot * 4, 4), 4)


def to_everyone(me, act):
    act(lax.rem(me + 1, DEVICES))

    def some(j, carry):
        for g in range(9):
            act(lax.rem(me + 2 + 9 * j + g, DEVICES))
        return carry

    lax.fori_loop(0, 14, some, 0)


def remote(src, dst, send, recv, device):
    return pltpu.make_async_remote_copy(
        src_ref=src, dst_ref=dst, send_sem=send, recv_sem=recv,
        device_id=(device,), device_id_type=MESH,
    )


def split3(x):
    hi = x.astype(BF16).astype(F32)
    rest = x - hi
    mid = rest.astype(BF16).astype(F32)
    return hi, mid, rest - mid


def setup_part(
    counts, links, map_ref, modes_ref, rhs_ref, goals,
    gathered, basis_out, modes_out, edge_out, rhs_out, inverse_out,
    padded, own, far, basis, halo_send, halo_recv, wide_send, wide_recv,
):
    me = lax.axis_index("dev")
    codes = map_ref[...]
    high = jnp.where(codes >= 0, codes >> 7, -1)
    low = jnp.where(codes >= 0, codes & 127, -1)
    column = iota((32, NMAX), 1)
    here = jnp.broadcast_to(high, (32, NMAX)) == iota((32, NMAX), 0)
    coarse_digit = jnp.where(here, column >> 6, 0).astype(F32).astype(BF16)
    fine_digit = jnp.where(here, column & 63, 0).astype(F32).astype(BF16)
    spots = (
        jnp.broadcast_to(low, (128, NMAX)) == iota((128, NMAX), 0)
    ).astype(F32).astype(BF16)
    digits = lax.dot_general(
        jnp.concatenate([coarse_digit, fine_digit], axis=0), spots,
        (((1,), (1,)), ((), ())), preferred_element_type=F32,
    )
    inverse = (digits[:32] * 64.0 + digits[32:]).astype(jnp.int32)
    inverse_out[...] = inverse[:CHUNKS]

    padded[...] = jnp.zeros_like(padded)
    for a in range(MODES):
        padded[a : a + 1, :] = modes_ref[a]
    for r in range(CHUNKS):
        face = r // 4
        live = iota((8, 128), 1) + (r % 4) * 128 < counts[0, face]
        row = inverse_out[r : r + 1, :]
        own[0, :, r * 128 : (r + 1) * 128] = jnp.where(live, permuted_chunk(padded, row), 0.0)
        own[1, :, r * 128 : (r + 1) * 128] = jnp.where(live, permuted_chunk(rhs_ref, row), 0.0)

    def exchange(which):
        return [
            remote(
                own.at[which, :, face_slice(face)], far.at[which, :, face_slice(OPPOSITE[face])],
                halo_send.at[which, face], halo_recv.at[which, OPPOSITE[face]],
                neighbour(me, FACE_STEPS[face]),
            )
            for face in range(FACES)
        ]

    pl.semaphore_wait(pltpu.get_barrier_semaphore(), DEVICES - 1)
    for copy in exchange(0) + exchange(1):
        copy.start()
    basis[...] = jnp.zeros_like(basis)
    basis[48:56, :] = own[0]
    basis[112:120, :] = own[0]
    modes_out[...] = own[0]
    for copy in exchange(0):
        copy.wait()
    for face in range(FACES):
        limit = jnp.where(links[0, face] >= 0, counts[0, face], 0)
        shared = iota((8, CAP), 1) < limit
        lanes = face_slice(face)
        edge = jnp.where(shared, -far[0, :, lanes], 0.0)
        basis[8 * face : 8 * face + 8, lanes] = edge
        basis[8 * face + 64 : 8 * face + 72, lanes] = edge
        edge_out[:, lanes] = edge

    row_block = lax.dot_general(
        own[0], basis[...], (((1,), (1,)), ((), ())),
        precision=HIGHEST, preferred_element_type=F32,
    )
    spot = iota((1, 128), 1)
    goal_row = jnp.zeros((1, 128), F32)
    for a in range(MODES):
        for l in range(LOADS):
            goal_row = jnp.where(spot == 16 * l + a, goals[0, a * LOADS + l], goal_row)
    packed = jnp.where(iota((3, 128), 1) < 64, row_block[0:3], row_block[3:6])
    gathered[slot_rows(me), :] = jnp.concatenate([packed, goal_row], axis=0)

    def start_send(device):
        part = gathered.at[slot_rows(me), :]
        remote(part, part, wide_send, wide_recv, device).start()

    to_everyone(me, start_send)
    top = basis[0:64, :]
    hi = top.astype(BF16)
    basis_out[0:64, :] = hi
    basis_out[64:128, :] = (top - hi.astype(F32)).astype(BF16)
    basis_out[128:192, :] = hi
    for copy in exchange(1):
        copy.wait()
    for face in range(FACES):
        limit = jnp.where(links[0, face] >= 0, counts[0, face], 0)
        shared = iota((8, CAP), 1) < limit
        lanes = face_slice(face)
        rhs_out[:, lanes] = own[1, :, lanes] - jnp.where(shared, far[1, :, lanes], 0.0)
    most = gathered.at[pl.ds(0, 4 * DEVICES - 4), :]
    remote(most, most, wide_send, wide_recv, lax.rem(me + 1, DEVICES)).wait()


def invert_together(blocks, layers):
    lane = iota((8, 128), 1)
    sub = iota((8, 128), 0)

    def spread(values, k):
        return jnp.broadcast_to(values[k : k + 1, :], (8, 128))

    def pair(n, carry):
        base = pl.multiple_of(n * 16, 16)
        pivots = [(half, k) for half in range(2) for k in range(MODES)]
        picks = [jnp.full((8, 128), base + 8 * half + k, jnp.int32) for half, k in pivots]
        group = lane >> 4
        inside = group == n
        panels = [
            [blocks[layer, pl.ds(base + 8 * half, 8), :] for half in range(2)] for layer in layers
        ]
        results = []
        for panel in panels:
            cols = [[lane_take(part, pick) for part in panel] for pick in picks]
            work = [
                jnp.where(inside, jnp.where(lane - base == sub + 8 * half, 1.0, 0.0), panel[half])
                for half in range(2)
            ]
            for p, (half, k) in enumerate(pivots):
                pivot = spread(cols[p][half], k)
                inv = pl.reciprocal(pivot, approx=True)
                inv = inv * (2.0 - pivot * inv)
                lift = list(cols[p])
                lift[half] = jnp.where(sub == k, lift[half] - 1.0, lift[half])
                lift = [part * inv for part in lift]
                for target in [work] + cols[p + 1 :]:
                    row = spread(target[half], k)
                    for other in range(2):
                        target[other] = target[other] - lift[other] * row
            results.append(jnp.concatenate(work, axis=0))
        for layer, panel, work in zip(layers, panels, results):
            column = jnp.concatenate([jnp.where(group < n, -part, part) for part in panel], axis=0)
            a, b, c = split3(column)
            d, e, f = split3(work)
            left = jnp.concatenate([a, a, b, a, c, b], axis=0).astype(BF16)
            right = jnp.concatenate([d, e, d, f, d, e], axis=0).astype(BF16)
            change = lax.dot_general(
                left, right, (((0,), (0,)), ((), ())), preferred_element_type=F32
            )
            clear = (iota((128, 128), 1) >> 4) == n
            blocks[layer] = jnp.where(clear, 0.0, blocks[layer]) - change
            blocks[layer, pl.ds(base, 16), :] = work
        return carry

    lax.fori_loop(0, 8, pair, 0)


def mm(a, b):
    return jnp.dot(a, b, precision=HIGHEST, preferred_element_type=F32)


def coarse_part(
    owner, links, rows, rows_kept_out, solver_out, ordered, blocks, up, down, fold, sel,
):
    lane = iota((8, 128), 1)
    sub = iota((8, 128), 0)
    offset = owner[0]
    me = lax.axis_index("dev")

    turned = rows[...]
    for bit in range(7):
        by = 4 << bit
        if by % 8:
            moved = pltpu.roll(turned, 4 * DEVICES - by, 0)
        else:
            moved = jnp.concatenate([turned[by:], turned[:by]], axis=0)
        turned = jnp.where(((offset >> bit) & 1) == 1, moved, turned)
    ordered[...] = turned

    def layer_rows(layer, carry):
        for n in range(16):
            slot = layer * 16 + n
            tile = jnp.broadcast_to(ordered[pl.ds(slot * 4 + 2, 1), :], (8, 128))
            for r in range(2):
                part = jnp.broadcast_to(ordered[pl.ds(slot * 4 + r, 1), :], (8, 128))
                tile = jnp.where((sub == r) | (sub == r + 3), part, tile)
            aside = jnp.where(sub < 3, 0, 64)
            real = sub < MODES
            apart = (lane >> 3) - n
            within = lane & 7
            face = jnp.where(apart == 0, 6, jnp.where(apart == -1, 0, jnp.where(
                apart == 1, 1, jnp.where(apart == -4, 2, jnp.where(apart == 4, 3, 7)))))
            linked = (face < 7) & real & (within < MODES)
            block = jnp.where(linked, lane_take(tile, ((face * 8 + within) & 63) + aside), 0.0)
            pad = (apart == 0) & (within == sub) & (sub >= MODES)
            blocks[layer, n * 8 : n * 8 + 8, :] = jnp.where(pad, 1.0, block)
            here = (apart == 0) & real & (within < MODES)
            up[layer, n * 8 : n * 8 + 8, :] = jnp.where(here, lane_take(tile, 40 + within + aside), 0.0)
            down[layer, n * 8 : n * 8 + 8, :] = jnp.where(here, lane_take(tile, 32 + within + aside), 0.0)
        return carry

    lax.fori_loop(0, 8, layer_rows, 0)

    own = (me - offset) & (DEVICES - 1)
    for f in range(7):
        target = own if f == 6 else links[0, f]
        for layer in range(8):
            hit = ((lane >> 3) + 16 * layer == target) & ((lane & 7) == sub) & (sub < MODES)
            sel[layer, 8 * f : 8 * f + 8, :] = jnp.where(hit, 1.0, 0.0)
    for layer in range(8):
        sel[layer, 56:64, :] = jnp.zeros((8, 128), F32)

    for k in range(3):
        low, high = k, 7 - k
        invert_together(blocks, (low, high))
        fold[low] = mm(blocks[low], up[low])
        fold[high] = mm(blocks[high], down[high])
        blocks[low + 1] = blocks[low + 1] - mm(down[low + 1], fold[low])
        blocks[high - 1] = blocks[high - 1] - mm(up[high - 1], fold[high])
        sel[low + 1] = sel[low + 1] - mm(sel[low], fold[low])
        sel[high - 1] = sel[high - 1] - mm(sel[high], fold[high])
    invert_together(blocks, (3,))
    fold[3] = mm(blocks[3], up[3])
    blocks[4] = blocks[4] - mm(down[4], fold[3])
    sel[4] = sel[4] - mm(sel[3], fold[3])
    invert_together(blocks, (4,))
    sel[4] = mm(sel[4], blocks[4])
    for k in range(3, -1, -1):
        sel[k] = mm(sel[k] - mm(sel[k + 1], down[k + 1]), blocks[k])
        if k < 3:
            j = 7 - k
            sel[j] = mm(sel[j] - mm(sel[j - 1], up[j - 1]), blocks[j])

    parts = []
    for layer in range(8):
        parts.append(jnp.concatenate(split3(sel[layer]), axis=0).astype(BF16))
    row = iota((128, 128), 0)
    col = iota((128, 128), 1)
    for k in range(MODES):
        total = jnp.zeros((192, 128), F32)
        for layer in range(8):
            slot = ((row >> 3) + 16 * layer + offset) & (DEVICES - 1)
            hot = jnp.where(((row & 7) == k) & (slot == col), 1.0, 0.0).astype(BF16)
            total = total + jnp.dot(parts[layer], hot, preferred_element_type=F32)
        values = total[0:64] + total[64:128] + total[128:192]
        hi = values.astype(BF16)
        solver_out[k * 64 : (k + 1) * 64, 0:128] = hi
        solver_out[k * 64 : (k + 1) * 64, 128:256] = hi
        solver_out[k * 64 : (k + 1) * 64, 256:384] = (values - hi.astype(F32)).astype(BF16)
    rows_kept_out[...] = rows[pl.ds(3, DEVICES, stride=4), :]


def gradients_part(
    counts, links, map_ref, inverse, modes, edge, rhs, basis, solver, goal, load,
    lambda_out, residual_out,
    dual, vec, low_vec, prod, image, far, lam, direction, applied, coarse, live, omega, table,
    halo_send, halo_recv, wide_send, wide_recv,
):
    me = lax.axis_index("dev")
    lane = iota((8, 128), 1)
    sub = iota((8, 128), 0)
    for face in range(FACES):
        spot = iota((8, CAP), 1)
        alive = jnp.where(spot < counts[0, face], 1.0, 0.0)
        limit = jnp.where(links[0, face] >= 0, counts[0, face], 0)
        both = jnp.where(spot < limit, 1.0, 0.0)
        live[:, face_slice(face)] = both
        omega[:, face_slice(face)] = alive - 0.5 * both

    def coarse_solve(even, odd):
        rows = jnp.concatenate([even, odd], axis=1)
        hi = rows.astype(BF16)
        lo = (rows - hi.astype(F32)).astype(BF16)
        out = jnp.dot(
            solver[...], jnp.concatenate([hi, lo, hi], axis=0), preferred_element_type=F32
        )
        total = jnp.zeros((64, 128), F32)
        place = iota((64, 128), 1) & 15
        for k in range(MODES):
            part = out[k * 64 : (k + 1) * 64]
            total = jnp.where(place == k, part[:, :128], total)
            total = jnp.where(place == k + 8, part[:, 128:], total)
        top = total.astype(BF16)
        rest = (total - top.astype(F32)).astype(BF16)
        pair = jnp.concatenate([top, rest], axis=1)
        triple = jnp.concatenate([pair, pair, pair], axis=0)
        group = jnp.where(
            ((iota((8, 256), 1) & 127) >> 4) == iota((8, 256), 0), 1.0, 0.0
        ).astype(BF16)
        return lax.dot_general(
            group, triple, (((1,), (1,)), ((), ())), preferred_element_type=F32
        )

    def expand(z3):
        top = z3.astype(BF16).astype(F32)
        packed = jnp.where(iota((8, 192), 1) < 128, top, z3 - top).astype(BF16)
        return jnp.dot(packed, basis[...], preferred_element_type=F32)

    def halo(parity):
        return [
            remote(
                image.at[:, face_slice(face)], far.at[parity, :, face_slice(OPPOSITE[face])],
                halo_send.at[parity, face], halo_recv.at[parity, OPPOSITE[face]],
                neighbour(me, FACE_STEPS[face]),
            )
            for face in range(FACES)
        ]

    def dual_apply(parity):
        def to_columns(o, carry):
            for g in range(GROUP):
                lanes = pl.ds(pl.multiple_of((o * GROUP + g) * 128, 128), 128)
                low_vec[:, lanes] = permuted_chunk(vec, map_ref[:, lanes]).astype(BF16)
            return carry

        lax.fori_loop(0, CHUNKS // GROUP, to_columns, 0)

        def product(n, carry):
            lanes = pl.ds(pl.multiple_of(n * 512, 512), 512)
            prod[:, lanes] = jnp.dot(low_vec[...], dual[:, lanes], preferred_element_type=F32)
            return carry

        lax.fori_loop(0, NMAX // 512, product, 0)

        def to_faces(o, carry):
            for g in range(GROUP):
                r = o * GROUP + g
                lanes = pl.ds(pl.multiple_of(r * 128, 128), 128)
                piece = permuted_chunk(prod, inverse[pl.ds(r, 1), :])
                image[:, lanes] = jnp.where(omega[:, lanes] > 0.0, piece, 0.0)
            return carry

        lax.fori_loop(0, CHUNKS // GROUP, to_faces, 0)
        for copy in halo(parity):
            copy.start()

    def assembled(parity):
        for copy in halo(parity):
            copy.wait()
        return image[...] - live[...] * far[parity]

    def share(parity, own, faces, extra):
        tiles = []
        for r in range(4):
            columns = list(enumerate(own)) + [(6 + k, e) for k, e in enumerate(extra)]
            if r > 0:
                columns = list(enumerate(faces[2 * r - 2]))
                columns += [(8 + k, e) for k, e in enumerate(faces[2 * r - 1])]
            tile = jnp.zeros((8, 128), F32)
            for k, values in columns:
                tile = jnp.where((lane & 15) == k, values, tile)
            tiles.append(jnp.sum(jnp.where((lane >> 4) == sub, tile, 0.0), axis=0, keepdims=True))
        table[parity, slot_rows(me), :] = jnp.concatenate(tiles, axis=0)

        def start_send(device):
            part = table.at[parity, slot_rows(me), :]
            remote(part, part, wide_send.at[parity], wide_recv.at[parity], device).start()

        to_everyone(me, start_send)
        most = table.at[parity, pl.ds(0, 4 * DEVICES - 4), :]
        everything = remote(
            most, most, wide_send.at[parity], wide_recv.at[parity], lax.rem(me + 1, DEVICES)
        )
        everything.wait()
        first = table[parity, pl.ds(0, DEVICES, stride=4), :]
        even, odd = first, jnp.zeros((DEVICES, 128), F32)
        for r in range(3):
            pair = table[parity, pl.ds(r + 1, DEVICES, stride=4), :]
            even = even + pltpu.roll(pair, FACE_STEPS[2 * r] % DEVICES, 0)
            odd = odd + pltpu.roll(pair, FACE_STEPS[2 * r + 1] % DEVICES, 0)
        return first, even, odd

    def mode_sums(values):
        return [
            jnp.sum(modes[a : a + 1, :] * values, axis=1, keepdims=True) for a in range(MODES)
        ]

    def face_sums(values):
        return [
            [
                jnp.sum(
                    edge[a : a + 1, face * CAP : (face + 1) * CAP]
                    * values[:, face * CAP : (face + 1) * CAP],
                    axis=1, keepdims=True,
                )
                for a in range(MODES)
            ]
            for face in range(FACES)
        ]

    def summed(product):
        return jnp.sum(product, axis=1, keepdims=True)

    def total_of(totals, k):
        return jnp.sum(jnp.where(lane == 16 * sub + k, totals, 0.0), axis=1, keepdims=True)

    start = expand(coarse_solve(goal[...], jnp.zeros((DEVICES, 128), F32)))
    lam[...] = start
    vec[...] = start
    load.wait()
    dual_apply(0)
    negative = -image[...]
    _, even, odd = share(0, mode_sums(rhs[...] + negative), face_sums(negative), [])
    z3 = coarse_solve(even, odd)
    vec[...] = rhs[...] - assembled(0) - expand(z3)
    direction[...] = jnp.zeros_like(direction)
    applied[...] = jnp.zeros_like(applied)
    coarse[...] = jnp.zeros_like(coarse)

    def iteration(step, carry):
        rho_old, curve_old = carry
        parity = lax.rem(step, 2)
        dual_apply(parity)
        w = vec[...]
        y = image[...]
        extra = [
            summed(omega[...] * w * w), summed(w * y), summed(omega[...] * w * applied[...]),
            summed(direction[...] * y),
        ]
        first, even, odd = share(parity, mode_sums(y), face_sums(y), extra)
        totals = jnp.broadcast_to(jnp.sum(first, axis=0, keepdims=True), (8, 128))
        rho = total_of(totals, 6)
        ratio = rho / rho_old
        curve = (
            total_of(totals, 7) + ratio * (total_of(totals, 8) + total_of(totals, 9))
            + ratio * ratio * curve_old
        )
        length = rho / curve
        z3 = coarse_solve(even, odd) + ratio * coarse[...]
        coarse[...] = z3
        image_of = assembled(parity) + ratio * applied[...]
        applied[...] = image_of
        way = vec[...] + ratio * direction[...]
        direction[...] = way
        lam[...] = lam[...] + length * way
        vec[...] = vec[...] - length * (image_of - expand(z3))
        return rho, curve

    far_off = jnp.full((8, 1), jnp.inf, F32)
    lax.fori_loop(1, ITERS + 1, iteration, (far_off, jnp.zeros((8, 1), F32)))

    def to_outputs(o, carry):
        for g in range(GROUP):
            lanes = pl.ds(pl.multiple_of((o * GROUP + g) * 128, 128), 128)
            row = map_ref[:, lanes]
            lambda_out[0, :, lanes] = permuted_chunk(lam, row)
            residual_out[0, :, lanes] = permuted_chunk(vec, row)
        return carry

    lax.fori_loop(0, CHUNKS // GROUP, to_outputs, 0)


def kernel(
    counts, links, owner, goals, map_hbm, modes_hbm, rhs_hbm, dual_hbm,
    lambda_out, residual_out,
    map_in, modes_in, rhs_in, input_sems,
    gathered, basis, modes, edge, rhs, inverse, padded, own, early_far, wide_basis,
    early_send, early_recv, rows_send, rows_recv,
    goal, solver, ordered, blocks, up, down, fold, sel,
    dual, dual_sem, *scratch,
):
    greet_all(lax.axis_index("dev"))
    inputs = [
        pltpu.make_async_copy(map_hbm, map_in, input_sems.at[0]),
        pltpu.make_async_copy(modes_hbm, modes_in, input_sems.at[1]),
        pltpu.make_async_copy(rhs_hbm.at[0], rhs_in, input_sems.at[2]),
    ]
    for copy in inputs:
        copy.start()
    load = pltpu.make_async_copy(dual_hbm.at[0], dual, dual_sem)
    load.start()
    for copy in inputs:
        copy.wait()
    setup_part(
        counts, links, map_in, modes_in, rhs_in, goals,
        gathered, basis, modes, edge, rhs, inverse,
        padded, own, early_far, wide_basis, early_send, early_recv, rows_send, rows_recv,
    )
    coarse_part(owner, links, gathered, goal, solver, ordered, blocks, up, down, fold, sel)
    gradients_part(
        counts, links, map_in, inverse, modes, edge, rhs, basis, solver, goal, load,
        lambda_out, residual_out, dual, *scratch,
    )


VM = pl.BlockSpec(memory_space=pltpu.VMEM)
SM = pl.BlockSpec(memory_space=pltpu.SMEM)
ANY = pl.BlockSpec(memory_space=pl.ANY)
DMA = pltpu.SemaphoreType.DMA


def vmem(*shape, dtype=F32):
    return pltpu.VMEM(shape, dtype)


def per_device(
    dual_blocks, rigid_modes, dual_local, coarse_rhs,
    iface_sizes, neighbours, shared_counts, iface_map, owner,
):
    out = jax.ShapeDtypeStruct((1, LOADS, NMAX), F32)
    return pl.pallas_call(
        kernel,
        out_shape=(out, out),
        in_specs=[SM] * 4 + [ANY] * 4,
        out_specs=(VM, VM),
        scratch_shapes=[
            vmem(1, NMAX, dtype=jnp.int32), vmem(MODES, 1, NMAX), vmem(8, NMAX), DMA((3,)),
            vmem(DEVICES * 4, 128), vmem(192, NMAX, dtype=BF16), vmem(8, NMAX), vmem(8, NMAX),
            vmem(8, NMAX), vmem(CHUNKS, 128, dtype=jnp.int32), vmem(8, NMAX), vmem(2, 8, NMAX),
            vmem(2, 8, NMAX), vmem(128, NMAX), DMA((2, 6)), DMA((2, 6)), DMA, DMA,
            vmem(DEVICES, 128), vmem(64 * MODES, 384, dtype=BF16), vmem(DEVICES * 4, 128),
            vmem(8, 128, 128), vmem(8, 128, 128), vmem(8, 128, 128), vmem(8, 128, 128),
            vmem(8, 64, 128),
            vmem(NMAX, NMAX, dtype=BF16), DMA,
            vmem(8, NMAX), vmem(8, NMAX, dtype=BF16), vmem(8, NMAX), vmem(8, NMAX),
            vmem(2, 8, NMAX), vmem(8, NMAX), vmem(8, NMAX), vmem(8, NMAX), vmem(8, 192),
            vmem(8, NMAX), vmem(8, NMAX), vmem(2, 4 * DEVICES, 128),
            DMA((2, 6)), DMA((2, 6)), DMA((2,)), DMA((2,)),
        ],
        compiler_params=pltpu.CompilerParams(
            collective_id=0, has_side_effects=True, vmem_limit_bytes=58 << 20
        ),
        name="feti",
    )(
        shared_counts, neighbours, owner, coarse_rhs.reshape(1, MODES * LOADS), iface_map,
        rigid_modes.transpose(1, 0, 2), dual_local, dual_blocks,
    )


def solution(mesh):
    in_specs = (
        P("dev", None, None), P("dev", None, None), P("dev", None, None), P("dev", None, None),
        P("dev"), P("dev", None), P("dev", None), P("dev", None), P(),
    )
    out_specs = (P("dev", None, None), P("dev", None, None))
    return jax.shard_map(
        per_device, mesh=mesh, in_specs=in_specs, out_specs=out_specs, check_vma=False
    )
```

```python
import functools

import jax
import jax.numpy as jnp
from jax import lax
from jax.experimental import pallas as pl
from jax.experimental.pallas import tpu as pltpu
from jax.sharding import PartitionSpec as P

FACES = 6
MODES = 6
CAP = 512
NMAX = 3072
LOADS = 8
CHUNKS = NMAX // 128
ITERS = 3
GROUP = 12
DEVICES = 128
OPPOSITE = (1, 0, 3, 2, 5, 4)
FACE_STEPS = (-1, 1, -4, 4, -16, 16)
HIGHEST = lax.Precision.HIGHEST
F32 = jnp.float32
BF16 = jnp.bfloat16
MESH = pl.DeviceIdType.MESH


def iota(shape, dim):
    return lax.broadcasted_iota(jnp.int32, shape, dim)


def lane_take(values, lanes):
    return jnp.take_along_axis(values, lanes, axis=1, mode="promise_in_bounds")


def permuted_chunk(src, index_row):
    index = jnp.broadcast_to(index_row, (8, 128))
    chunk = index >> 7
    lanes = index & 127
    out = jnp.zeros((8, 128), F32)
    for s in range(CHUNKS):
        piece = lane_take(src[:, s * 128 : (s + 1) * 128], lanes)
        out = jnp.where(chunk == s, piece, out)
    return out


def neighbour(me, step):
    return lax.rem(me + step + DEVICES, DEVICES)


def face_slice(face):
    return pl.ds(face * CAP, CAP)


def greet_all(me):
    barrier = pltpu.get_barrier_semaphore()

    to_everyone(me, lambda device: pl.semaphore_signal(
        barrier, inc=1, device_id=(device,), device_id_type=MESH
    ))


def slot_rows(slot):
    return pl.ds(pl.multiple_of(slot * 4, 4), 4)


def to_everyone(me, act):
    q = lax.rem(me, 8)
    x = lax.rem(me // 8, 4)
    y = me // 32

    def at(dy, dx, dq):
        return (lax.rem(y + dy, 4) * 4 + lax.rem(x + dx, 4)) * 8 + lax.rem(q + dq, 8)

    order = (4, 5, 3, 2, 6, 1, 7, 0)
    for dy in (2, 1, 3):

        def some(i, carry, dy=dy):
            for dq in order:
                act(at(dy, i + 2, dq))
            return carry

        lax.fori_loop(0, 4, some, 0)
    for dx in (2, 1, 3, 0):
        for dq in order:
            if dx or dq:
                act(at(0, dx, dq))


def remote(src, dst, send, recv, device):
    return pltpu.make_async_remote_copy(
        src_ref=src, dst_ref=dst, send_sem=send, recv_sem=recv,
        device_id=(device,), device_id_type=MESH,
    )


def split3(x):
    hi = x.astype(BF16).astype(F32)
    rest = x - hi
    mid = rest.astype(BF16).astype(F32)
    return hi, mid, rest - mid


def setup_part(
    counts, links, map_ref, modes_ref, rhs_ref, goals,
    gathered, basis_out, modes_out, edge_out, rhs_out, inverse_out,
    padded, own, far, basis, halo_send, halo_recv, wide_send, wide_recv,
):
    me = lax.axis_index("dev")
    codes = map_ref[...]
    high = jnp.where(codes >= 0, codes >> 7, -1)
    low = jnp.where(codes >= 0, codes & 127, -1)
    column = iota((32, NMAX), 1)
    here = jnp.broadcast_to(high, (32, NMAX)) == iota((32, NMAX), 0)
    coarse_digit = jnp.where(here, column >> 6, 0).astype(F32).astype(BF16)
    fine_digit = jnp.where(here, column & 63, 0).astype(F32).astype(BF16)
    spots = (
        jnp.broadcast_to(low, (128, NMAX)) == iota((128, NMAX), 0)
    ).astype(F32).astype(BF16)
    digits = lax.dot_general(
        jnp.concatenate([coarse_digit, fine_digit], axis=0), spots,
        (((1,), (1,)), ((), ())), preferred_element_type=F32,
    )
    inverse = (digits[:32] * 64.0 + digits[32:]).astype(jnp.int32)
    inverse_out[...] = inverse[:CHUNKS]

    padded[...] = jnp.zeros_like(padded)
    for a in range(MODES):
        padded[a : a + 1, :] = modes_ref[a]
    for r in range(CHUNKS):
        face = r // 4
        live = iota((8, 128), 1) + (r % 4) * 128 < counts[0, face]
        row = inverse_out[r : r + 1, :]
        own[0, :, r * 128 : (r + 1) * 128] = jnp.where(live, permuted_chunk(padded, row), 0.0)
        own[1, :, r * 128 : (r + 1) * 128] = jnp.where(live, permuted_chunk(rhs_ref, row), 0.0)

    def exchange(which):
        return [
            remote(
                own.at[which, :, face_slice(face)], far.at[which, :, face_slice(OPPOSITE[face])],
                halo_send.at[which, face], halo_recv.at[which, OPPOSITE[face]],
                neighbour(me, FACE_STEPS[face]),
            )
            for face in range(FACES)
        ]

    pl.semaphore_wait(pltpu.get_barrier_semaphore(), DEVICES - 1)
    for copy in exchange(0) + exchange(1):
        copy.start()
    basis[...] = jnp.zeros_like(basis)
    basis[48:56, :] = own[0]
    basis[112:120, :] = own[0]
    modes_out[...] = own[0]
    for copy in exchange(0):
        copy.wait()
    for face in range(FACES):
        limit = jnp.where(links[0, face] >= 0, counts[0, face], 0)
        shared = iota((8, CAP), 1) < limit
        lanes = face_slice(face)
        edge = jnp.where(shared, -far[0, :, lanes], 0.0)
        basis[8 * face : 8 * face + 8, lanes] = edge
        basis[8 * face + 64 : 8 * face + 72, lanes] = edge
        edge_out[:, lanes] = edge

    row_block = lax.dot_general(
        own[0], basis[...], (((1,), (1,)), ((), ())),
        precision=HIGHEST, preferred_element_type=F32,
    )
    spot = iota((1, 128), 1)
    goal_row = jnp.zeros((1, 128), F32)
    for a in range(MODES):
        for l in range(LOADS):
            goal_row = jnp.where(spot == 16 * l + a, goals[a, 0, l], goal_row)
    packed = jnp.where(iota((3, 128), 1) < 64, row_block[0:3], row_block[3:6])
    gathered[slot_rows(me), :] = jnp.concatenate([packed, goal_row], axis=0)

    def start_send(device):
        part = gathered.at[slot_rows(me), :]
        remote(part, part, wide_send, wide_recv, device).start()

    to_everyone(me, start_send)
    top = basis[0:64, :]
    hi = top.astype(BF16)
    basis_out[0:64, :] = hi
    basis_out[64:128, :] = (top - hi.astype(F32)).astype(BF16)
    basis_out[128:192, :] = hi
    for copy in exchange(1):
        copy.wait()
    for face in range(FACES):
        limit = jnp.where(links[0, face] >= 0, counts[0, face], 0)
        shared = iota((8, CAP), 1) < limit
        lanes = face_slice(face)
        rhs_out[:, lanes] = own[1, :, lanes] - jnp.where(shared, far[1, :, lanes], 0.0)
    most = gathered.at[pl.ds(0, 4 * DEVICES - 4), :]
    remote(most, most, wide_send, wide_recv, lax.rem(me + 1, DEVICES)).wait()


def invert_together(blocks, layers):
    lane = iota((8, 128), 1)
    sub = iota((8, 128), 0)

    def spread(values, k):
        return jnp.broadcast_to(values[k : k + 1, :], (8, 128))

    def pair(n, carry):
        base = pl.multiple_of(n * 16, 16)
        pivots = [(half, k) for half in range(2) for k in range(MODES)]
        picks = [jnp.full((8, 128), base + 8 * half + k, jnp.int32) for half, k in pivots]
        group = lane >> 4
        inside = group == n
        panels = [
            [blocks[layer, pl.ds(base + 8 * half, 8), :] for half in range(2)] for layer in layers
        ]
        results = []
        for panel in panels:
            cols = [[lane_take(part, pick) for part in panel] for pick in picks]
            work = [
                jnp.where(inside, jnp.where(lane - base == sub + 8 * half, 1.0, 0.0), panel[half])
                for half in range(2)
            ]
            for p, (half, k) in enumerate(pivots):
                pivot = spread(cols[p][half], k)
                inv = pl.reciprocal(pivot, approx=True)
                inv = inv * (2.0 - pivot * inv)
                lift = list(cols[p])
                lift[half] = jnp.where(sub == k, lift[half] - 1.0, lift[half])
                lift = [part * inv for part in lift]
                for target in [work] + cols[p + 1 :]:
                    row = spread(target[half], k)
                    for other in range(2):
                        target[other] = target[other] - lift[other] * row
            results.append(jnp.concatenate(work, axis=0))
        for layer, panel, work in zip(layers, panels, results):
            column = jnp.concatenate([jnp.where(group < n, -part, part) for part in panel], axis=0)
            a, b, c = split3(column)
            d, e, f = split3(work)
            left = jnp.concatenate([a, a, b, a, c, b], axis=0).astype(BF16)
            right = jnp.concatenate([d, e, d, f, d, e], axis=0).astype(BF16)
            change = lax.dot_general(
                left, right, (((0,), (0,)), ((), ())), preferred_element_type=F32
            )
            clear = (iota((128, 128), 1) >> 4) == n
            blocks[layer] = jnp.where(clear, 0.0, blocks[layer]) - change
            blocks[layer, pl.ds(base, 16), :] = work
        return carry

    lax.fori_loop(0, 8, pair, 0)


def mm(a, b):
    return jnp.dot(a, b, precision=HIGHEST, preferred_element_type=F32)


def coarse_part(
    owner, links, rows, rows_kept_out, solver_out, ordered, blocks, up, down, fold, sel,
):
    lane = iota((8, 128), 1)
    sub = iota((8, 128), 0)
    offset = owner[0]
    me = lax.axis_index("dev")

    turned = rows[...]
    for bit in range(7):
        by = 4 << bit
        if by % 8:
            moved = pltpu.roll(turned, 4 * DEVICES - by, 0)
        else:
            moved = jnp.concatenate([turned[by:], turned[:by]], axis=0)
        turned = jnp.where(((offset >> bit) & 1) == 1, moved, turned)
    ordered[...] = turned

    def layer_rows(layer, carry):
        for n in range(16):
            slot = layer * 16 + n
            tile = jnp.broadcast_to(ordered[pl.ds(slot * 4 + 2, 1), :], (8, 128))
            for r in range(2):
                part = jnp.broadcast_to(ordered[pl.ds(slot * 4 + r, 1), :], (8, 128))
                tile = jnp.where((sub == r) | (sub == r + 3), part, tile)
            aside = jnp.where(sub < 3, 0, 64)
            real = sub < MODES
            apart = (lane >> 3) - n
            within = lane & 7
            face = jnp.where(apart == 0, 6, jnp.where(apart == -1, 0, jnp.where(
                apart == 1, 1, jnp.where(apart == -4, 2, jnp.where(apart == 4, 3, 7)))))
            linked = (face < 7) & real & (within < MODES)
            block = jnp.where(linked, lane_take(tile, ((face * 8 + within) & 63) + aside), 0.0)
            pad = (apart == 0) & (within == sub) & (sub >= MODES)
            blocks[layer, n * 8 : n * 8 + 8, :] = jnp.where(pad, 1.0, block)
            here = (apart == 0) & real & (within < MODES)
            up[layer, n * 8 : n * 8 + 8, :] = jnp.where(here, lane_take(tile, 40 + within + aside), 0.0)
            down[layer, n * 8 : n * 8 + 8, :] = jnp.where(here, lane_take(tile, 32 + within + aside), 0.0)
        return carry

    lax.fori_loop(0, 8, layer_rows, 0)

    own = (me - offset) & (DEVICES - 1)
    for f in range(7):
        target = own if f == 6 else links[0, f]
        for layer in range(8):
            hit = ((lane >> 3) + 16 * layer == target) & ((lane & 7) == sub) & (sub < MODES)
            sel[layer, 8 * f : 8 * f + 8, :] = jnp.where(hit, 1.0, 0.0)
    for layer in range(8):
        sel[layer, 56:64, :] = jnp.zeros((8, 128), F32)

    for k in range(3):
        low, high = k, 7 - k
        invert_together(blocks, (low, high))
        fold[low] = mm(blocks[low], up[low])
        fold[high] = mm(blocks[high], down[high])
        blocks[low + 1] = blocks[low + 1] - mm(down[low + 1], fold[low])
        blocks[high - 1] = blocks[high - 1] - mm(up[high - 1], fold[high])
        sel[low + 1] = sel[low + 1] - mm(sel[low], fold[low])
        sel[high - 1] = sel[high - 1] - mm(sel[high], fold[high])
    invert_together(blocks, (3,))
    fold[3] = mm(blocks[3], up[3])
    blocks[4] = blocks[4] - mm(down[4], fold[3])
    sel[4] = sel[4] - mm(sel[3], fold[3])
    invert_together(blocks, (4,))
    sel[4] = mm(sel[4], blocks[4])
    for k in range(3, -1, -1):
        sel[k] = mm(sel[k] - mm(sel[k + 1], down[k + 1]), blocks[k])
        if k < 3:
            j = 7 - k
            sel[j] = mm(sel[j] - mm(sel[j - 1], up[j - 1]), blocks[j])

    parts = []
    for layer in range(8):
        parts.append(jnp.concatenate(split3(sel[layer]), axis=0).astype(BF16))
    row = iota((128, 128), 0)
    col = iota((128, 128), 1)
    for k in range(MODES):
        total = jnp.zeros((192, 128), F32)
        for layer in range(8):
            slot = ((row >> 3) + 16 * layer + offset) & (DEVICES - 1)
            hot = jnp.where(((row & 7) == k) & (slot == col), 1.0, 0.0).astype(BF16)
            total = total + jnp.dot(parts[layer], hot, preferred_element_type=F32)
        values = total[0:64] + total[64:128] + total[128:192]
        hi = values.astype(BF16)
        solver_out[k * 64 : (k + 1) * 64, 0:128] = hi
        solver_out[k * 64 : (k + 1) * 64, 128:256] = hi
        solver_out[k * 64 : (k + 1) * 64, 256:384] = (values - hi.astype(F32)).astype(BF16)
    rows_kept_out[...] = rows[pl.ds(3, DEVICES, stride=4), :]


def gradients_part(
    counts, links, map_ref, inverse, modes, edge, rhs, basis, solver, goal, load,
    both_out,
    dual, vec, low_vec, prod, image, far, lam, direction, applied, coarse, live, omega, table,
    halo_send, halo_recv, wide_send, wide_recv,
):
    me = lax.axis_index("dev")
    lane = iota((8, 128), 1)
    sub = iota((8, 128), 0)
    for face in range(FACES):
        spot = iota((8, CAP), 1)
        alive = jnp.where(spot < counts[0, face], 1.0, 0.0)
        limit = jnp.where(links[0, face] >= 0, counts[0, face], 0)
        both = jnp.where(spot < limit, 1.0, 0.0)
        live[:, face_slice(face)] = both
        omega[:, face_slice(face)] = alive - 0.5 * both

    def coarse_solve(even, odd):
        rows = jnp.concatenate([even, odd], axis=1)
        hi = rows.astype(BF16)
        lo = (rows - hi.astype(F32)).astype(BF16)
        out = jnp.dot(
            solver[...], jnp.concatenate([hi, lo, hi], axis=0), preferred_element_type=F32
        )
        total = jnp.zeros((64, 128), F32)
        place = iota((64, 128), 1) & 15
        for k in range(MODES):
            part = out[k * 64 : (k + 1) * 64]
            total = jnp.where(place == k, part[:, :128], total)
            total = jnp.where(place == k + 8, part[:, 128:], total)
        top = total.astype(BF16)
        rest = (total - top.astype(F32)).astype(BF16)
        pair = jnp.concatenate([top, rest], axis=1)
        triple = jnp.concatenate([pair, pair, pair], axis=0)
        group = jnp.where(
            ((iota((8, 256), 1) & 127) >> 4) == iota((8, 256), 0), 1.0, 0.0
        ).astype(BF16)
        return lax.dot_general(
            group, triple, (((1,), (1,)), ((), ())), preferred_element_type=F32
        )

    def expand(z3):
        top = z3.astype(BF16).astype(F32)
        packed = jnp.where(iota((8, 192), 1) < 128, top, z3 - top).astype(BF16)
        return jnp.dot(packed, basis[...], preferred_element_type=F32)

    def halo(parity):
        return [
            remote(
                image.at[:, face_slice(face)], far.at[parity, :, face_slice(OPPOSITE[face])],
                halo_send.at[parity, face], halo_recv.at[parity, OPPOSITE[face]],
                neighbour(me, FACE_STEPS[face]),
            )
            for face in range(FACES)
        ]

    def dual_apply(parity):
        def to_columns(o, carry):
            for g in range(GROUP):
                lanes = pl.ds(pl.multiple_of((o * GROUP + g) * 128, 128), 128)
                low_vec[:, lanes] = permuted_chunk(vec, map_ref[:, lanes]).astype(BF16)
            return carry

        lax.fori_loop(0, CHUNKS // GROUP, to_columns, 0)

        def product(n, carry):
            lanes = pl.ds(pl.multiple_of(n * 512, 512), 512)
            prod[:, lanes] = jnp.dot(low_vec[...], dual[:, lanes], preferred_element_type=F32)
            return carry

        lax.fori_loop(0, NMAX // 512, product, 0)

        def to_faces(o, carry):
            for g in range(GROUP):
                r = o * GROUP + g
                lanes = pl.ds(pl.multiple_of(r * 128, 128), 128)
                piece = permuted_chunk(prod, inverse[pl.ds(r, 1), :])
                image[:, lanes] = jnp.where(omega[:, lanes] > 0.0, piece, 0.0)
            return carry

        lax.fori_loop(0, CHUNKS // GROUP, to_faces, 0)
        for copy in halo(parity):
            copy.start()

    def assembled(parity):
        for copy in halo(parity):
            copy.wait()
        return image[...] - live[...] * far[parity]

    def share(parity, own, faces, extra):
        tiles = []
        for r in range(4):
            columns = list(enumerate(own)) + [(6 + k, e) for k, e in enumerate(extra)]
            if r > 0:
                columns = list(enumerate(faces[2 * r - 2]))
                columns += [(8 + k, e) for k, e in enumerate(faces[2 * r - 1])]
            tile = jnp.zeros((8, 128), F32)
            for k, values in columns:
                tile = jnp.where((lane & 15) == k, values, tile)
            tiles.append(jnp.sum(jnp.where((lane >> 4) == sub, tile, 0.0), axis=0, keepdims=True))
        table[parity, slot_rows(me), :] = jnp.concatenate(tiles, axis=0)

        def start_send(device):
            part = table.at[parity, slot_rows(me), :]
            remote(part, part, wide_send.at[parity], wide_recv.at[parity], device).start()

        to_everyone(me, start_send)
        most = table.at[parity, pl.ds(0, 4 * DEVICES - 4), :]
        everything = remote(
            most, most, wide_send.at[parity], wide_recv.at[parity], lax.rem(me + 1, DEVICES)
        )
        everything.wait()
        first = table[parity, pl.ds(0, DEVICES, stride=4), :]
        even, odd = first, jnp.zeros((DEVICES, 128), F32)
        for r in range(3):
            pair = table[parity, pl.ds(r + 1, DEVICES, stride=4), :]
            even = even + pltpu.roll(pair, FACE_STEPS[2 * r] % DEVICES, 0)
            odd = odd + pltpu.roll(pair, FACE_STEPS[2 * r + 1] % DEVICES, 0)
        return first, even, odd

    def mode_sums(values):
        return [
            jnp.sum(modes[a : a + 1, :] * values, axis=1, keepdims=True) for a in range(MODES)
        ]

    def face_sums(values):
        return [
            [
                jnp.sum(
                    edge[a : a + 1, face * CAP : (face + 1) * CAP]
                    * values[:, face * CAP : (face + 1) * CAP],
                    axis=1, keepdims=True,
                )
                for a in range(MODES)
            ]
            for face in range(FACES)
        ]

    def summed(product):
        return jnp.sum(product, axis=1, keepdims=True)

    def total_of(totals, k):
        return jnp.sum(jnp.where(lane == 16 * sub + k, totals, 0.0), axis=1, keepdims=True)

    start = expand(coarse_solve(goal[...], jnp.zeros((DEVICES, 128), F32)))
    lam[...] = start
    vec[...] = start
    load.wait()
    dual_apply(0)
    negative = -image[...]
    _, even, odd = share(0, mode_sums(rhs[...] + negative), face_sums(negative), [])
    z3 = coarse_solve(even, odd)
    vec[...] = rhs[...] - assembled(0) - expand(z3)
    direction[...] = jnp.zeros_like(direction)
    applied[...] = jnp.zeros_like(applied)
    coarse[...] = jnp.zeros_like(coarse)

    def iteration(step, carry):
        rho_old, curve_old = carry
        parity = lax.rem(step, 2)
        dual_apply(parity)
        w = vec[...]
        y = image[...]
        extra = [
            summed(omega[...] * w * w), summed(w * y), summed(omega[...] * w * applied[...]),
            summed(direction[...] * y),
        ]
        first, even, odd = share(parity, mode_sums(y), face_sums(y), extra)
        totals = jnp.broadcast_to(jnp.sum(first, axis=0, keepdims=True), (8, 128))
        rho = total_of(totals, 6)
        ratio = rho / rho_old
        curve = (
            total_of(totals, 7) + ratio * (total_of(totals, 8) + total_of(totals, 9))
            + ratio * ratio * curve_old
        )
        length = rho / curve
        z3 = coarse_solve(even, odd) + ratio * coarse[...]
        coarse[...] = z3
        image_of = assembled(parity) + ratio * applied[...]
        applied[...] = image_of
        way = vec[...] + ratio * direction[...]
        direction[...] = way
        lam[...] = lam[...] + length * way
        vec[...] = vec[...] - length * (image_of - expand(z3))
        return rho, curve

    far_off = jnp.full((8, 1), jnp.inf, F32)
    lax.fori_loop(1, ITERS + 1, iteration, (far_off, jnp.zeros((8, 1), F32)))

    def to_outputs(o, carry):
        for g in range(GROUP):
            lanes = pl.ds(pl.multiple_of((o * GROUP + g) * 128, 128), 128)
            row = map_ref[:, lanes]
            both_out[0, :, lanes] = permuted_chunk(lam, row)
            both_out[1, :, lanes] = permuted_chunk(vec, row)
        return carry

    lax.fori_loop(0, CHUNKS // GROUP, to_outputs, 0)


def kernel(
    counts, links, owner, goals, map_hbm, modes_hbm, rhs_hbm, dual_hbm,
    both_out,
    map_in, modes_in, rhs_in, input_sems,
    gathered, basis, modes, edge, rhs, inverse, padded, own, early_far, wide_basis,
    early_send, early_recv, rows_send, rows_recv,
    goal, solver, ordered, blocks, up, down, fold, sel,
    dual, dual_sem, *scratch,
):
    greet_all(lax.axis_index("dev"))
    inputs = [
        pltpu.make_async_copy(map_hbm, map_in, input_sems.at[0]),
        pltpu.make_async_copy(modes_hbm, modes_in, input_sems.at[1]),
        pltpu.make_async_copy(rhs_hbm.at[0], rhs_in, input_sems.at[2]),
    ]
    for copy in inputs:
        copy.start()
    load = pltpu.make_async_copy(dual_hbm.at[0], dual, dual_sem)
    load.start()
    for copy in inputs:
        copy.wait()
    setup_part(
        counts, links, map_in, modes_in, rhs_in, goals,
        gathered, basis, modes, edge, rhs, inverse,
        padded, own, early_far, wide_basis, early_send, early_recv, rows_send, rows_recv,
    )
    coarse_part(owner, links, gathered, goal, solver, ordered, blocks, up, down, fold, sel)
    gradients_part(
        counts, links, map_in, inverse, modes, edge, rhs, basis, solver, goal, load,
        both_out, dual, *scratch,
    )


VM = pl.BlockSpec(memory_space=pltpu.VMEM)
SM = pl.BlockSpec(memory_space=pltpu.SMEM)
ANY = pl.BlockSpec(memory_space=pl.ANY)
DMA = pltpu.SemaphoreType.DMA


def vmem(*shape, dtype=F32):
    return pltpu.VMEM(shape, dtype)


def per_device(
    dual_blocks, rigid_modes, dual_local, coarse_rhs,
    iface_sizes, neighbours, shared_counts, iface_map, owner,
):
    out = jax.ShapeDtypeStruct((2, LOADS, NMAX), F32)
    both = pl.pallas_call(
        kernel,
        out_shape=out,
        in_specs=[SM] * 4 + [ANY] * 4,
        out_specs=VM,
        scratch_shapes=[
            vmem(1, NMAX, dtype=jnp.int32), vmem(MODES, 1, NMAX), vmem(8, NMAX), DMA((3,)),
            vmem(DEVICES * 4, 128), vmem(192, NMAX, dtype=BF16), vmem(8, NMAX), vmem(8, NMAX),
            vmem(8, NMAX), vmem(CHUNKS, 128, dtype=jnp.int32), vmem(8, NMAX), vmem(2, 8, NMAX),
            vmem(2, 8, NMAX), vmem(128, NMAX), DMA((2, 6)), DMA((2, 6)), DMA, DMA,
            vmem(DEVICES, 128), vmem(64 * MODES, 384, dtype=BF16), vmem(DEVICES * 4, 128),
            vmem(8, 128, 128), vmem(8, 128, 128), vmem(8, 128, 128), vmem(8, 128, 128),
            vmem(8, 64, 128),
            vmem(NMAX, NMAX, dtype=BF16), DMA,
            vmem(8, NMAX), vmem(8, NMAX, dtype=BF16), vmem(8, NMAX), vmem(8, NMAX),
            vmem(2, 8, NMAX), vmem(8, NMAX), vmem(8, NMAX), vmem(8, NMAX), vmem(8, 192),
            vmem(8, NMAX), vmem(8, NMAX), vmem(2, 4 * DEVICES, 128),
            DMA((2, 6)), DMA((2, 6)), DMA((2,)), DMA((2,)),
        ],
        compiler_params=pltpu.CompilerParams(
            collective_id=0, has_side_effects=True, vmem_limit_bytes=58 << 20
        ),
        name="feti",
    )(
        shared_counts, neighbours, owner, coarse_rhs.transpose(1, 0, 2), iface_map,
        rigid_modes.transpose(1, 0, 2), dual_local, dual_blocks,
    )
    return both[0:1], both[1:2]


def solution(mesh):
    in_specs = (
        P("dev", None, None), P("dev", None, None), P("dev", None, None), P("dev", None, None),
        P("dev"), P("dev", None), P("dev", None), P("dev", None), P(),
    )
    out_specs = (P("dev", None, None), P("dev", None, None))
    return jax.shard_map(
        per_device, mesh=mesh, in_specs=in_specs, out_specs=out_specs, check_vma=False
    )
```
